256 devices in a mesh: pts: 32 (over x, y, core), wid: 8 (over z).
Axes of the slice: x: 4, y: 4, z: 8, core: 2. Of those that a mesh axis runs over, the one named last changes fastest.
Arguments:
- vertex_features: bfloat16 [360448, 512], P('pts'), may hold values from -40 to 40, as said below
- entry_matrix: bfloat16 [512, 512], P(None, 'wid'), may hold values from -2 to 2, as said below
- partition_matrix: bfloat16 [64, 32], replicated, may hold values from -3 to 3, as said below
- sharpness_matrix: float32 [64], replicated, may hold values from -3 to 3, as said below
- summary_qkv_matrix: float32 [3, 64, 64], replicated, may hold values from -3 to 3
- exit_matrix: bfloat16 [512, 512], P('wid'), may hold values from -0.5 to 0.5
- widening_matrix: bfloat16 [512, 512], P('wid'), may hold values from -0.25 to 0.25
- narrowing_matrix: bfloat16 [512, 512], P('wid'), may hold values from -0.25 to 0.25
Outputs:
- result: bfloat16 [360448, 512], P(('pts', 'wid'))
The draws below stay inside these ranges and needn't reach their ends.
Inputs may be any that keep to these rules, and one draw needn't show every extreme that they name: `vertex_features`: features of the points, of order one to ten. `entry_matrix`: weights of the point projection. `partition_matrix`: slice logit weights. `sharpness_matrix`: temperature weights.
All inputs are finite; a program needn't handle non-finite values.
Results may differ from the reference program's by a relative error of at most 0.013.
Values may be sent and summed in bfloat16 or wider, within the bound.
A program may use at most 128 MiB of HBM per device.

```python
import jax
import jax.numpy as jnp
from jax import lax

D = 512
H = 8
DH = 64
G = 32
FF = 512
NPOINTS = 360448


def draw_vertex_features(key, part):
    key_base = jax.random.fold_in(key, 11)
    key_dir = jax.random.fold_in(key, 12)
    key_scale = jax.random.fold_in(key, 13)
    base = jnp.clip(jax.random.normal(key_base, (NPOINTS, D), jnp.float32), -4.0, 4.0)
    spread = jnp.exp(jax.random.uniform(key_scale, (NPOINTS, 1), jnp.float32, 0.0, 1.1))
    direction = jnp.clip(jax.random.normal(key_dir, (1, D), jnp.float32), -4.0, 4.0)
    ramp = 1.0 + 2.0 * jnp.arange(NPOINTS, dtype=jnp.float32)[:, None] / jnp.float32(max(NPOINTS - 1, 1))
    values = base * jnp.minimum(spread, 3.0) + ramp * direction
    values = 0.5 * values
    return jnp.clip(values, -40.0, 40.0).astype(jnp.bfloat16)


def draw_entry_matrix(key, part):
    noise = jnp.clip(jax.random.normal(jax.random.fold_in(key, 21), (D, D), jnp.float32), -6.0, 6.0) / jnp.sqrt(jnp.float32(D))
    return jnp.clip(noise, -2.0, 2.0).astype(jnp.bfloat16)


def draw_partition_matrix(key, part):
    rough = jax.random.normal(jax.random.fold_in(key, 31), (DH, G), jnp.float32)
    values = 0.8 * rough
    return jnp.clip(values, -3.0, 3.0).astype(jnp.bfloat16)


def draw_sharpness_matrix(key, part):
    rough = jax.random.normal(jax.random.fold_in(key, 41), (DH,), jnp.float32)
    values = 0.6 * rough
    return jnp.clip(values, -3.0, 3.0).astype(jnp.float32)


def draw_summary_qkv_matrix(key, part):
    rough = jax.random.normal(jax.random.fold_in(key, 51), (3, DH, DH), jnp.float32)
    values = 0.55 * rough
    return jnp.clip(values, -3.0, 3.0).astype(jnp.float32)


def block_scale(rng, shape, shards, least, top_value):
    level = 1.0
    for axis_at, parts in shards:
        steps = jax.random.uniform(jax.random.fold_in(jax.random.fold_in(rng, 6), axis_at), (parts,), jnp.float32, least / len(shards), top_value / len(shards))
        level = level * jnp.repeat(jnp.exp(steps), shape[axis_at] // parts).reshape((-1,) + (1,) * (len(shape) - 1 - axis_at))
    return level


def normal_values(stream_key, extent, deviation, most, pieces=(), held_as=jnp.bfloat16):
    result = jax.random.normal(stream_key, extent, jnp.float32) * deviation
    if len(pieces) > 0:
        result = block_scale(stream_key, extent, pieces, -0.22, 0.18) * result
    return jnp.clip(result, min=-most, max=most).astype(held_as)


def setup_inputs(seed: int = 0) -> dict:
    arg_keys = jax.random.split(jax.random.key(seed), 9)
    return {
        "vertex_features": draw_vertex_features(jax.random.fold_in(arg_keys[8], 71), 0),
        "entry_matrix": draw_entry_matrix(jax.random.fold_in(arg_keys[8], 71), 0),
        "partition_matrix": draw_partition_matrix(jax.random.fold_in(arg_keys[8], 71), 0),
        "sharpness_matrix": draw_sharpness_matrix(jax.random.fold_in(arg_keys[8], 71), 0),
        "summary_qkv_matrix": draw_summary_qkv_matrix(jax.random.fold_in(arg_keys[8], 71), 0),
        "exit_matrix": normal_values(arg_keys[5], (D, D), (D // 4) ** -0.5, 0.5, ((0, 8),)),
        "widening_matrix": normal_values(arg_keys[6], (D, FF), D ** -0.5, 0.25, ((0, 8),)),
        "narrowing_matrix": normal_values(arg_keys[7], (FF, D), FF ** -0.5, 0.25, ((0, 8),)),
    }


def layer_norm(values):
    centred = values - lax.optimization_barrier(jnp.mean(values, axis=-1, keepdims=True))
    variance = lax.optimization_barrier(jnp.mean(centred * centred, axis=-1, keepdims=True))
    return centred * lax.rsqrt(variance + 1e-05)

def reference(vertex_features, entry_matrix, partition_matrix, sharpness_matrix, summary_qkv_matrix, exit_matrix, widening_matrix, narrowing_matrix):
    features = vertex_features.astype(jnp.float32)
    normed = layer_norm(features).astype(jnp.bfloat16)
    feats = jnp.dot(normed, entry_matrix, preferred_element_type=jnp.float32).astype(jnp.bfloat16)
    attention_cluster = feats.reshape(feats.shape[0], H, DH).astype(jnp.float32)
    partition_sharpness = 0.5 + jax.nn.softplus(jnp.einsum('kgv,v->kg', attention_cluster, sharpness_matrix))
    partition_scores = jnp.einsum('nhd,dg->nhg', attention_cluster, partition_matrix.astype(jnp.float32))
    partition_mapping = jax.nn.softmax(partition_scores / partition_sharpness[:, :, None], axis=-1).astype(jnp.bfloat16)
    weights32 = partition_mapping.astype(jnp.float32)
    numerator = jnp.einsum('nhg,nhd->hgd', weights32, attention_cluster)
    mass = lax.optimization_barrier(jnp.sum(weights32, axis=0))
    token_rows = numerator / (mass[:, :, None] + 1e-05)
    hp = lax.Precision.HIGHEST
    queries = jnp.einsum('hgd,de->hge', token_rows, summary_qkv_matrix[0], precision=hp)
    keys_all = jnp.einsum('hgd,de->hge', token_rows, summary_qkv_matrix[1], precision=hp)
    value_rows_total = jnp.einsum('hgd,de->hge', token_rows, summary_qkv_matrix[2], precision=hp)
    scores = jnp.einsum('hge,hke->hgk', queries, keys_all, precision=hp) / jnp.sqrt(jnp.float32(DH))
    attend = jax.nn.softmax(scores, axis=-1)
    out_tok = jnp.einsum('hgk,hke->hge', attend, value_rows_total, precision=hp).astype(jnp.bfloat16)
    deslice = jnp.einsum('nhg,hgd->nhd', weights32, out_tok.astype(jnp.float32)).astype(jnp.bfloat16)
    deslice = deslice.reshape(feats.shape[0], D)
    midway = features + jnp.dot(deslice, exit_matrix, preferred_element_type=jnp.float32)
    normed2 = layer_norm(midway).astype(jnp.bfloat16)
    hidden = jax.nn.gelu(jnp.dot(normed2, widening_matrix, preferred_element_type=jnp.float32)).astype(jnp.bfloat16)
    return (midway + jnp.dot(hidden, narrowing_matrix, preferred_element_type=jnp.float32)).astype(jnp.bfloat16)
```

```python
import functools

import jax
import jax.numpy as jnp
from jax import lax
from jax.experimental import pallas as pl
from jax.experimental.pallas import tpu as pltpu
from jax.sharding import PartitionSpec as P

MESH = pl.DeviceIdType.MESH
F32, BF16 = jnp.float32, jnp.bfloat16
HIGH = lax.Precision.HIGHEST

D, H, DH, G = 512, 8, 64, 32
ROWS = 11264
OWN = 1408
BLK = 1024
NBLK = ROWS // BLK
TBLK = 352
HALF = DH // 2

X_PEERS = [(dx, dc) for dx in range(4) for dc in range(2)]


def contract_lanes(a, b, precision=None):
    return lax.dot_general(
        a, b, (((1,), (1,)), ((), ())), preferred_element_type=F32, precision=precision
    )


def softmax_weights(logits, temperature_logit):
    soft = jnp.maximum(temperature_logit, 0.0) + jnp.log(1.0 + jnp.exp(-jnp.abs(temperature_logit)))
    scaled = logits * (1.0 / (0.5 + soft))
    e = jnp.exp(scaled - jnp.max(scaled, axis=0, keepdims=True))
    return (e * (1.0 / jnp.sum(e, axis=0, keepdims=True))).astype(BF16)


def kernel(
    x_hbm, entry_hbm, part_ref, sharp_ref, qkv_ref, exit_hbm, wide_hbm, narrow_hbm,
    out_hbm,
    xv, eh, waug, pT, cs, mu_s, rs_s, yT0, yT1, acc, wall, yall, wT, wn, mbuf, outv,
    xbuf, ybuf, zbuf,
    x_sem, in_sem, out_sem,
    ring_send, ring_recv, d2d_send, d2d_recv,
    xs_send, xs_recv, ys_send, ys_recv, zs_send, zs_recv,
):
    pts, z = lax.axis_index("pts"), lax.axis_index("wid")
    core = lax.rem(pts, 2)
    gx, gy = pts // 8, lax.rem(pts // 2, 4)
    partner = pts + 1 - 2 * core

    def pts_at(dx, dy, dc):
        return (lax.rem(gx + dx, 4) * 4 + lax.rem(gy + dy, 4)) * 2 + lax.rem(core + dc, 2)

    def z_at(dz):
        return lax.rem(z + dz + H, H)

    def x_copy(i):
        return pltpu.make_async_copy(
            x_hbm.at[pl.ds(i * BLK, BLK)], xv.at[pl.ds(i * BLK, BLK)], x_sem.at[i]
        )

    entry_copy = pltpu.make_async_copy(entry_hbm, eh, in_sem.at[0])
    entry_copy.start()
    for i in range(NBLK):
        x_copy(i).start()
    own_copies = []
    for k, ref in ((1, exit_hbm), (2, wide_hbm), (3, narrow_hbm)):
        for c in range(2):
            own_copies.append(
                pltpu.make_async_copy(
                    ref.at[pl.ds(c * HALF, HALF)], wall.at[k, z, c], in_sem.at[2 * k - 1 + c]
                )
            )
    for copy in own_copies:
        copy.start()

    barrier = pltpu.get_barrier_semaphore()
    for dx, dc in X_PEERS[1:]:
        pl.semaphore_signal(barrier, inc=1, device_id=(pts_at(dx, 0, dc), z), device_id_type=MESH)
    for dy in range(1, 4):
        pl.semaphore_signal(barrier, inc=1, device_id=(pts_at(0, dy, 0), z), device_id_type=MESH)
    for dz in range(1, H):
        pl.semaphore_signal(barrier, inc=1, device_id=(pts, z_at(dz)), device_id_type=MESH)

    partT = part_ref[...].astype(F32).T.astype(BF16)
    sharp = jnp.broadcast_to(sharp_ref[...], (16, DH))
    sharp_hi = sharp.astype(BF16).astype(F32)
    row16 = lax.broadcasted_iota(jnp.int32, (16, DH), 0)
    tail = jnp.where(row16 == 0, sharp_hi, jnp.where(row16 == 1, sharp - sharp_hi, 0.0))
    pT[0:G, :] = partT
    pT[G : G + 16, :] = tail.astype(BF16)

    entry_copy.wait()
    ehT = eh[...].astype(F32).T
    ehT_bf = ehT.astype(BF16)
    wall[0, z] = ehT_bf.reshape(2, HALF, D)
    cs[...] = jnp.broadcast_to(jnp.sum(ehT, axis=1, keepdims=True), (DH, 128))
    rowd = lax.broadcasted_iota(jnp.int32, (DH, D), 0)
    waug[...] = jnp.concatenate([ehT, jnp.where(rowd == 0, 1.0 / D, 0.0)], axis=0).T.astype(BF16)
    acc[...] = jnp.zeros_like(acc)
    ones16 = jnp.ones((16, BLK), BF16)

    def part_of(g, shard, half, d, s):
        rows = pl.ds(0, HALF) if s < 4 else (pl.ds(0, HALF // 2) if d > 0 else pl.ds(HALF // 2, HALF // 2))
        mats = pl.ds(0, 1) if g == 0 else pl.ds(1, 3)
        return wall.at[mats, shard, half, rows]

    def ring(g, d, s):
        ref = part_of(g, z_at(-d * (s - 1)), core, d, s)
        at = (g, (1 - d) // 2, s - 1)
        return pltpu.make_async_remote_copy(
            src_ref=ref, dst_ref=ref, send_sem=ring_send.at[at], recv_sem=ring_recv.at[at],
            device_id=(pts, z_at(d)), device_id_type=MESH,
        )

    def arrival(g, d, s):
        ref = part_of(g, z_at(-d * s), core, d, s)
        at = (g, (1 - d) // 2, s - 1)
        return pltpu.make_async_remote_copy(
            src_ref=ref, dst_ref=ref, send_sem=ring_send.at[at], recv_sem=ring_recv.at[at],
            device_id=(pts, z_at(d)), device_id_type=MESH,
        )

    def to_partner(g, d, s):
        ref = part_of(g, z_at(-d * s), core, d, s)
        at = (g, (1 - d) // 2, s - 1)
        return pltpu.make_async_remote_copy(
            src_ref=ref, dst_ref=ref, send_sem=d2d_send.at[at], recv_sem=d2d_recv.at[at],
            device_id=(partner, z), device_id_type=MESH,
        )

    def from_partner(g, d, s):
        ref = part_of(g, z_at(-d * s), 1 - core, d, s)
        at = (g, (1 - d) // 2, s - 1)
        return pltpu.make_async_remote_copy(
            src_ref=ref, dst_ref=ref, send_sem=d2d_send.at[at], recv_sem=d2d_recv.at[at],
            device_id=(partner, z), device_id_type=MESH,
        )

    def ring_start():
        for copy in own_copies:
            copy.wait()
        pl.semaphore_wait(barrier, 7 + 3 + 7)
        for g in range(2):
            for d in (1, -1):
                ring(g, d, 1).start()

    def ring_step(g, s):
        for d in (1, -1):
            arrival(g, d, s).wait_recv()
            if s < 4:
                ring(g, d, s + 1).start()
            to_partner(g, d, s).start()

    def project(i, yT):
        x_copy(i).wait()
        xb = xv[pl.ds(pl.multiple_of(i * BLK, BLK), BLK), :]
        y = jnp.dot(xb, waug[...], preferred_element_type=F32)
        xf = xb.astype(F32)
        sq = xf * xf
        sq = (sq[:, 0:128] + sq[:, 128:256]) + (sq[:, 256:384] + sq[:, 384:512])
        total = jnp.sum(sq, axis=1, keepdims=True)
        lane = lax.broadcasted_iota(jnp.int32, (BLK, 128), 1)
        yT[...] = jnp.where(lane == DH + 1, total, y).T

    def slices(i, yT):
        mean = yT[DH : DH + 1, :]
        var = jnp.maximum(yT[DH + 1 : DH + 2, :] * (1.0 / D) - mean * mean, 0.0)
        rstd = lax.rsqrt(var + 1e-05)
        lanes = pl.ds(pl.multiple_of(i * BLK, BLK), BLK)
        mu_s[:, lanes] = mean
        rs_s[:, lanes] = rstd
        feats = ((yT[0:DH, :] - cs[:, 0:1] * mean) * rstd).astype(BF16)
        logits = jnp.dot(pT[...], feats, preferred_element_type=F32)
        w = softmax_weights(logits[0:G], logits[G : G + 1] + logits[G + 1 : G + 2])
        acc[...] += contract_lanes(jnp.concatenate([feats, ones16], axis=0), w)

    project(0, yT0)

    def two_blocks(j, _):
        @pl.when(j == 2)
        def _():
            ring_start()

        @pl.when(j == 4)
        def _():
            ring_step(0, 1)

        slices(2 * j, yT0)
        project(2 * j + 1, yT1)
        slices(2 * j + 1, yT1)
        project(2 * j + 2, yT0)
        return 0

    lax.fori_loop(0, NBLK // 2, two_blocks, 0)
    slices(NBLK - 1, yT0)

    xbuf[0] = jnp.concatenate([acc[...], jnp.zeros((48, G), F32)], axis=0).T

    def x_send(r):
        dx, dc = X_PEERS[r]
        return pltpu.make_async_remote_copy(
            src_ref=xbuf.at[0], dst_ref=xbuf.at[r], send_sem=xs_send.at[r], recv_sem=xs_recv.at[r],
            device_id=(pts_at(dx, 0, dc), z), device_id_type=MESH,
        )

    def y_send(r):
        return pltpu.make_async_remote_copy(
            src_ref=ybuf.at[0], dst_ref=ybuf.at[r], send_sem=ys_send.at[r], recv_sem=ys_recv.at[r],
            device_id=(pts_at(0, r, 0), z), device_id_type=MESH,
        )

    for r in range(1, 8):
        x_send(r).start()
    ring_step(0, 2)
    ring_step(1, 1)
    ring_step(0, 3)
    for r in range(1, 8):
        x_send(r).wait_recv()
    ybuf[0] = jnp.sum(xbuf[...], axis=0)
    for r in range(1, 4):
        y_send(r).start()
    ring_step(1, 2)
    ring_step(0, 4)

    for s in range(1, 5):
        for d in (1, -1):
            from_partner(0, d, s).wait_recv()
    own = pl.multiple_of(z * OWN, 128)
    entryT = wall[0].reshape(D, D)
    yall[...] = contract_lanes(entryT, xv[pl.ds(own, OWN), :])
    colsum = jnp.sum(entryT.astype(F32), axis=1, keepdims=True)
    mean_own = mu_s[:, pl.ds(own, OWN)]
    yall[...] = (yall[...] - colsum * mean_own) * rs_s[:, pl.ds(own, OWN)]
    ring_step(1, 3)

    def own_head(h, _):
        feats = yall[pl.ds(pl.multiple_of(h * DH, DH), DH), :].astype(BF16)
        logits = jnp.dot(pT[...], feats, preferred_element_type=F32)
        w = softmax_weights(logits[0:G], logits[G : G + 1] + logits[G + 1 : G + 2])
        wT[pl.ds(pl.multiple_of(h * G, G), G), :] = w
        return 0

    lax.fori_loop(0, H, own_head, 0)
    wn[...] = wT[...].T

    for r in range(1, 4):
        y_send(r).wait_recv()
    sums = jnp.sum(ybuf[...], axis=0)
    tokens = sums[:, 0:DH] / (sums[:, DH : DH + 1] + 1e-05)
    queries = jnp.dot(tokens, qkv_ref[0], preferred_element_type=F32, precision=HIGH)
    keys = jnp.dot(tokens, qkv_ref[1], preferred_element_type=F32, precision=HIGH)
    values = jnp.dot(
        tokens, jnp.concatenate([qkv_ref[2], jnp.zeros((DH, DH), F32)], axis=1),
        preferred_element_type=F32, precision=HIGH,
    )
    scores = contract_lanes(queries, keys, precision=HIGH) * 0.125
    e = jnp.exp(scores - jnp.max(scores, axis=1, keepdims=True))
    attend = e / jnp.sum(e, axis=1, keepdims=True)
    zbuf[z] = jnp.dot(attend, values, preferred_element_type=F32, precision=HIGH).astype(BF16)

    def z_send(dz):
        return pltpu.make_async_remote_copy(
            src_ref=zbuf.at[z], dst_ref=zbuf.at[z], send_sem=zs_send.at[dz], recv_sem=zs_recv.at[dz],
            device_id=(pts, z_at(dz)), device_id_type=MESH,
        )

    def z_arrival(dz):
        at = zbuf.at[z_at(-dz)]
        return pltpu.make_async_remote_copy(
            src_ref=at, dst_ref=at, send_sem=zs_send.at[dz], recv_sem=zs_recv.at[dz],
            device_id=(pts, z_at(dz)), device_id_type=MESH,
        )

    for dz in range(1, H):
        z_send(dz).start()
    ring_step(1, 4)
    for s in range(1, 5):
        for d in (1, -1):
            from_partner(1, d, s).wait_recv()
    for dz in range(1, H):
        z_arrival(dz).wait_recv()

    for h in range(H):
        mbuf[h * G : (h + 1) * G, :] = jnp.dot(
            zbuf[h][:, 0:DH], wall[1, h].reshape(DH, D), preferred_element_type=F32
        ).astype(BF16)

    def out_copy(t):
        rows = pl.ds(t * TBLK, TBLK)
        return pltpu.make_async_copy(outv.at[rows], out_hbm.at[rows], out_sem.at[t])

    def tail_rows(t, _):
        rows = pl.ds(pl.multiple_of(t * TBLK, 32), TBLK)
        x_rows = xv[pl.ds(pl.multiple_of(own + t * TBLK, 32), TBLK), :].astype(F32)
        midway = x_rows + jnp.dot(wn[rows, :], mbuf[...], preferred_element_type=F32)
        centred = midway - jnp.mean(midway, axis=1, keepdims=True)
        var = jnp.mean(centred * centred, axis=1, keepdims=True)
        normed = (centred * lax.rsqrt(var + 1e-05)).astype(BF16)
        hidden = jnp.dot(normed, wall[2].reshape(D, D), preferred_element_type=F32)
        hidden = jax.nn.gelu(hidden).astype(BF16)
        out = midway + jnp.dot(hidden, wall[3].reshape(D, D), preferred_element_type=F32)
        outv[rows, :] = out.astype(BF16)
        out_copy(t).start()
        return 0

    lax.fori_loop(0, OWN // TBLK, tail_rows, 0)

    for g in range(2):
        for d in (1, -1):
            for s in range(1, 5):
                ring(g, d, s).wait_send()
                to_partner(g, d, s).wait_send()
    for r in range(1, 8):
        x_send(r).wait_send()
    for r in range(1, 4):
        y_send(r).wait_send()
    for dz in range(1, H):
        z_send(dz).wait_send()
    for t in range(OWN // TBLK):
        out_copy(t).wait()


def local(x, entry, partition, sharpness, qkv, exit_matrix, widening, narrowing):
    hbm = pl.BlockSpec(memory_space=pl.ANY)
    vmem = pl.BlockSpec(memory_space=pltpu.VMEM)
    dma = pltpu.SemaphoreType.DMA
    return pl.pallas_call(
        kernel,
        out_shape=jax.ShapeDtypeStruct((OWN, D), BF16),
        in_specs=[hbm, hbm, vmem, vmem, vmem, hbm, hbm, hbm],
        out_specs=hbm,
        scratch_shapes=[
            pltpu.VMEM((ROWS, D), BF16),
            pltpu.VMEM((D, DH), BF16),
            pltpu.VMEM((D, 128), BF16),
            pltpu.VMEM((G + 16, DH), BF16),
            pltpu.VMEM((DH, 128), F32),
            pltpu.VMEM((1, ROWS), F32),
            pltpu.VMEM((1, ROWS), F32),
            pltpu.VMEM((128, BLK), F32),
            pltpu.VMEM((128, BLK), F32),
            pltpu.VMEM((DH + 16, G), F32),
            pltpu.VMEM((4, H, 2, HALF, D), BF16),
            pltpu.VMEM((D, OWN), F32),
            pltpu.VMEM((H * G, OWN), BF16),
            pltpu.VMEM((OWN, H * G), BF16),
            pltpu.VMEM((H * G, D), BF16),
            pltpu.VMEM((OWN, D), BF16),
            pltpu.VMEM((8, G, 128), F32),
            pltpu.VMEM((4, G, 128), F32),
            pltpu.VMEM((H, G, 128), BF16),
            dma((NBLK,)),
            dma((8,)),
            dma((OWN // TBLK,)),
            dma((2, 2, 4)),
            dma((2, 2, 4)),
            dma((2, 2, 4)),
            dma((2, 2, 4)),
            dma((8,)),
            dma((8,)),
            dma((4,)),
            dma((4,)),
            dma((8,)),
            dma((8,)),
        ],
        compiler_params=pltpu.CompilerParams(
            collective_id=0, has_side_effects=True, vmem_limit_bytes=60 * 2**20
        ),
    )(x, entry, partition, sharpness.reshape(1, DH), qkv, exit_matrix, widening, narrowing)


def solution(mesh):
    placed = (
        P("pts", None), P(None, "wid"), P(), P(), P(),
        P("wid", None), P("wid", None), P("wid", None),
    )
    return jax.shard_map(
        local, mesh=mesh, in_specs=placed, out_specs=P(("pts", "wid"), None), check_vma=False
    )
```

```python
import functools

import jax
import jax.numpy as jnp
from jax import lax
from jax.experimental import pallas as pl
from jax.experimental.pallas import tpu as pltpu
from jax.sharding import PartitionSpec as P

MESH = pl.DeviceIdType.MESH
F32, BF16 = jnp.float32, jnp.bfloat16
HIGH = lax.Precision.HIGHEST

D, H, DH, G = 512, 8, 64, 32
ROWS = 11264
OWN = 1408
BLK = 1024
NBLK = ROWS // BLK
TBLK = 352
HALF = DH // 2

PLANE = [(dx, dy) for dx in range(4) for dy in range(4)]
Z_NEAR = (1, -1, 2, -2)
Z_FAR = ((-2, 1, (0, HALF)), (2, -1, (0, HALF)), (-2, 2, (0, HALF // 2)), (2, -2, (HALF // 2, HALF // 2)))


def contract_lanes(a, b, precision=None):
    return lax.dot_general(
        a, b, (((1,), (1,)), ((), ())), preferred_element_type=F32, precision=precision
    )


def softmax_weights(logits, temperature_logit):
    soft = jnp.maximum(temperature_logit, 0.0) + jnp.log(1.0 + jnp.exp(-jnp.abs(temperature_logit)))
    scaled = logits * (1.0 / (0.5 + soft))
    e = jnp.exp(scaled - jnp.max(scaled, axis=0, keepdims=True))
    return (e * (1.0 / jnp.sum(e, axis=0, keepdims=True))).astype(BF16)


def kernel(
    x_hbm, entry_hbm, part_ref, sharp_ref, qkv_ref, exit_hbm, wide_hbm, narrow_hbm,
    out_ref,
    xv, eh, waug, pT, cs, f0, f1, acc, wall, nown, wT, wn, mbuf, yall,
    pair, plane, zbuf,
    x_sem, in_sem, own_sem, far_sem, d2d_sem, pair_sem, plane_sem, z_sem,
):
    pts, z = lax.axis_index("pts"), lax.axis_index("wid")
    core = lax.rem(pts, 2)
    gx, gy = pts // 8, lax.rem(pts // 2, 4)
    partner = pts + 1 - 2 * core

    def pts_at(dx, dy):
        return (lax.rem(gx + dx, 4) * 4 + lax.rem(gy + dy, 4)) * 2 + core

    def z_at(dz):
        return lax.rem(z + dz + H, H)

    def x_copy(i):
        return pltpu.make_async_copy(
            x_hbm.at[pl.ds(i * BLK, BLK)], xv.at[pl.ds(i * BLK, BLK)], x_sem.at[i]
        )

    entry_copy = pltpu.make_async_copy(entry_hbm, eh, in_sem.at[0])
    entry_copy.start()
    x_copy(0).start()
    own_copies = []
    for k, ref in enumerate((entry_hbm, exit_hbm, wide_hbm, narrow_hbm)):
        for c in range(2):
            own_copies.append(
                pltpu.make_async_copy(
                    ref.at[pl.ds(c * HALF, HALF)], wall.at[k, z, c], in_sem.at[1 + 2 * k + c]
                )
            )

    barrier = pltpu.get_barrier_semaphore()
    pl.semaphore_signal(barrier, inc=1, device_id=(partner, z), device_id_type=MESH)
    for dx, dy in PLANE[1:]:
        pl.semaphore_signal(barrier, inc=1, device_id=(pts_at(dx, dy), z), device_id_type=MESH)
    for dz in range(1, H):
        pl.semaphore_signal(barrier, inc=1, device_id=(pts, z_at(dz)), device_id_type=MESH)

    sharp = jnp.broadcast_to(sharp_ref[...], (16, DH))
    sharp_hi = sharp.astype(BF16).astype(F32)
    row16 = lax.broadcasted_iota(jnp.int32, (16, DH), 0)
    tail = jnp.where(row16 == 0, sharp_hi, jnp.where(row16 == 1, sharp - sharp_hi, 0.0))
    table = jnp.concatenate([part_ref[...].astype(F32), tail], axis=0)
    pT[...] = jnp.concatenate([table, jnp.zeros((G + 16, DH), F32)], axis=1).astype(BF16)
    acc[...] = jnp.zeros_like(acc)
    one_at_64 = (lax.broadcasted_iota(jnp.int32, (1, 128), 1) == DH).astype(F32)

    entry_copy.wait()
    for i in range(1, NBLK):
        x_copy(i).start()
    for copy in own_copies:
        copy.start()
    head = jnp.concatenate([eh[...].astype(F32), jnp.zeros((DH, D), F32)], axis=0).T
    cs[...] = jnp.sum(head, axis=0, keepdims=True)
    waug[:, 0:128] = head.astype(BF16)
    waug[:, 128:256] = jnp.full((D, 128), 1.0 / D, BF16)

    mats = (pl.ds(0, 1), pl.ds(1, 3))

    def to(ref, sems, device, target=None):
        return pltpu.make_async_remote_copy(
            src_ref=ref, dst_ref=ref if target is None else target, send_sem=sems.at[0], recv_sem=sems.at[1],
            device_id=device, device_id_type=MESH,
        )

    def half_of(g, offset, half, rows=pl.ds(0, HALF)):
        return wall.at[mats[g], z_at(offset), half, rows]

    def of_size(g, n, sems):
        return to(wall.at[mats[g], pl.ds(0, n), 0], sems.at[g], (partner, z))

    def weights_start():
        for copy in own_copies:
            copy.wait()
        for g in range(2):
            for dz in Z_NEAR:
                to(half_of(g, 0, core), own_sem.at[g], (pts, z_at(dz))).start()

    def weights_onward(g):
        of_size(g, 4, own_sem).wait_recv()
        for source, dz, rows in Z_FAR:
            to(half_of(g, source, core, pl.ds(*rows)), far_sem.at[g], (pts, z_at(dz))).start()
        for offset in Z_NEAR:
            to(half_of(g, offset, core), d2d_sem.at[g], (partner, z)).start()

    def weights_far(g):
        of_size(g, 3, far_sem).wait_recv()
        for offset in (3, -3, 4):
            to(half_of(g, offset, core), d2d_sem.at[g], (partner, z)).start()

    def weights_done(g):
        of_size(g, 7, d2d_sem).wait_recv()

    def project(i, fbuf):
        x_copy(i).wait()
        xb = xv[pl.ds(pl.multiple_of(i * BLK, BLK), BLK), :]
        y = jnp.dot(xb, waug[...], preferred_element_type=F32)
        xf = xb.astype(F32)
        sq = xf * xf
        sq = (sq[:, 0:128] + sq[:, 128:256]) + (sq[:, 256:384] + sq[:, 384:512])
        mean = y[:, 128:256]
        var = jnp.maximum(jnp.sum(sq, axis=1, keepdims=True) * (1.0 / D) - mean * mean, 0.0)
        feats = (y[:, 0:128] - cs[...] * mean) * lax.rsqrt(var + 1e-05)
        fbuf[...] = (feats + one_at_64).astype(BF16)

    def slices(fbuf):
        feats = fbuf[...]
        logits = contract_lanes(pT[...], feats)
        w = softmax_weights(logits[0:G], logits[G : G + 1] + logits[G + 1 : G + 2])
        acc[...] += jnp.dot(w, feats, preferred_element_type=F32)

    project(0, f0)

    def two_blocks(j, _):
        @pl.when(j == 1)
        def _():
            pl.semaphore_wait(barrier, 1 + 15 + 7)
            weights_start()

        slices(f0)
        project(2 * j + 1, f1)
        slices(f1)
        project(2 * j + 2, f0)
        return 0

    lax.fori_loop(0, NBLK // 2, two_blocks, 0)
    slices(f0)

    pair[0] = acc[...]
    pair_copy = to(pair.at[0], pair_sem, (partner, z), pair.at[1])
    pair_copy.start()
    weights_onward(0)
    pair_copy.wait_recv()
    plane[0] = pair[0] + pair[1]
    for r in range(1, 16):
        to(plane.at[0], plane_sem, (pts_at(*PLANE[r]), z), plane.at[r]).start()
    plane_all = to(plane.at[pl.ds(1, 15)], plane_sem, (partner, z))

    own = pl.multiple_of(z * OWN, 128)

    def own_norm(t, _):
        rows = xv[pl.ds(pl.multiple_of(own + t * 128, 128), 128), :].astype(F32)
        centred = rows - jnp.mean(rows, axis=1, keepdims=True)
        var = jnp.mean(centred * centred, axis=1, keepdims=True)
        nown[pl.ds(pl.multiple_of(t * 128, 128), 128), :] = (centred * lax.rsqrt(var + 1e-05)).astype(BF16)
        return 0

    lax.fori_loop(0, OWN // 128, own_norm, 0)
    weights_onward(1)
    weights_far(0)
    weights_done(0)
    yall[...] = contract_lanes(wall[0].reshape(D, D), nown[...]).astype(BF16)

    plane_all.wait_recv()
    sums = jnp.sum(plane[...], axis=0)
    tokens = sums[:, 0:DH] / (sums[:, DH : DH + 1] + 1e-05)
    queries = jnp.dot(tokens, qkv_ref[0], preferred_element_type=F32, precision=HIGH)
    keys = jnp.dot(tokens, qkv_ref[1], preferred_element_type=F32, precision=HIGH)
    values = jnp.dot(
        tokens, jnp.concatenate([qkv_ref[2], jnp.zeros((DH, DH), F32)], axis=1),
        preferred_element_type=F32, precision=HIGH,
    )
    scores = contract_lanes(queries, keys, precision=HIGH) * 0.125
    e = jnp.exp(scores - jnp.max(scores, axis=1, keepdims=True))
    attend = e / jnp.sum(e, axis=1, keepdims=True)
    zbuf[z] = jnp.dot(attend, values, preferred_element_type=F32, precision=HIGH).astype(BF16)

    for dz in range(1, H):
        to(zbuf.at[z], z_sem, (pts, z_at(dz))).start()
    z_all = to(zbuf.at[pl.ds(0, H - 1)], z_sem, (partner, z))

    def own_head(h, _):
        feats = yall[pl.ds(pl.multiple_of(h * DH, DH), DH), :]
        logits = jnp.dot(pT[:, 0:DH], feats, preferred_element_type=F32)
        w = softmax_weights(logits[0:G], logits[G : G + 1] + logits[G + 1 : G + 2])
        wT[pl.ds(pl.multiple_of(h * G, G), G), :] = w
        return 0

    lax.fori_loop(0, H, own_head, 0)
    weights_far(1)
    wn[...] = wT[...].T
    weights_done(1)
    z_all.wait_recv()

    for h in range(H):
        mbuf[h * G : (h + 1) * G, :] = jnp.dot(
            zbuf[h][:, 0:DH], wall[1, h].reshape(DH, D), preferred_element_type=F32
        ).astype(BF16)

    def tail_rows(t, _):
        rows = pl.ds(pl.multiple_of(t * TBLK, 32), TBLK)
        x_rows = xv[pl.ds(pl.multiple_of(own + t * TBLK, 32), TBLK), :].astype(F32)
        midway = x_rows + jnp.dot(wn[rows, :], mbuf[...], preferred_element_type=F32)
        centred = midway - jnp.mean(midway, axis=1, keepdims=True)
        var = jnp.mean(centred * centred, axis=1, keepdims=True)
        normed = (centred * lax.rsqrt(var + 1e-05)).astype(BF16)
        hidden = jnp.dot(normed, wall[2].reshape(D, D), preferred_element_type=F32)
        hidden = jax.nn.gelu(hidden).astype(BF16)
        out = midway + jnp.dot(hidden, wall[3].reshape(D, D), preferred_element_type=F32)
        out_ref[rows, :] = out.astype(BF16)
        return 0

    lax.fori_loop(0, OWN // TBLK, tail_rows, 0)

    for g in range(2):
        of_size(g, 4, own_sem).wait_send()
        of_size(g, 3, far_sem).wait_send()
        of_size(g, 7, d2d_sem).wait_send()
    pair_copy.wait_send()
    plane_all.wait_send()
    z_all.wait_send()


OUT = pltpu.VMEM((OWN, D), BF16)


def local(x, entry, partition, sharpness, qkv, exit_matrix, widening, narrowing):
    hbm = pl.BlockSpec(memory_space=pl.ANY)
    vmem = pl.BlockSpec(memory_space=pltpu.VMEM)
    dma = pltpu.SemaphoreType.DMA
    return pl.pallas_call(
        kernel,
        out_shape=OUT,
        in_specs=[hbm, hbm, vmem, vmem, vmem, hbm, hbm, hbm],
        out_specs=vmem,
        scratch_shapes=[
            pltpu.VMEM((ROWS, D), BF16),
            pltpu.VMEM((DH, D), BF16),
            pltpu.VMEM((D, 256), BF16),
            pltpu.VMEM((G + 16, 128), BF16),
            pltpu.VMEM((1, 128), F32),
            pltpu.VMEM((BLK, 128), BF16),
            pltpu.VMEM((BLK, 128), BF16),
            pltpu.VMEM((G, 128), F32),
            pltpu.VMEM((4, H, 2, HALF, D), BF16),
            pltpu.VMEM((OWN, D), BF16),
            pltpu.VMEM((H * G, OWN), BF16),
            pltpu.VMEM((OWN, H * G), BF16),
            pltpu.VMEM((H * G, D), BF16),
            pltpu.VMEM((D, OWN), BF16),
            pltpu.VMEM((2, G, 128), F32),
            pltpu.VMEM((16, G, 128), F32),
            pltpu.VMEM((H, G, 128), BF16),
            dma((NBLK,)),
            dma((9,)),
            dma((2, 2)),
            dma((2, 2)),
            dma((2, 2)),
            dma((2,)),
            dma((2,)),
            dma((2,)),
        ],
        compiler_params=pltpu.CompilerParams(
            collective_id=0, has_side_effects=True, vmem_limit_bytes=60 * 2**20
        ),
    )(x, entry.T, partition.T, sharpness.reshape(1, DH), qkv, exit_matrix, widening, narrowing)


def solution(mesh):
    placed = (
        P("pts", None), P(None, "wid"), P(), P(), P(),
        P("wid", None), P("wid", None), P("wid", None),
    )
    return jax.shard_map(
        local, mesh=mesh, in_specs=placed, out_specs=P(("pts", "wid"), None), check_vma=False
    )
```

```python
import functools

import jax
import jax.numpy as jnp
from jax import lax
from jax.experimental import pallas as pl
from jax.experimental.pallas import tpu as pltpu
from jax.sharding import PartitionSpec as P

MESH = pl.DeviceIdType.MESH
F32, BF16 = jnp.float32, jnp.bfloat16
HIGH = lax.Precision.HIGHEST

D, H, DH, G = 512, 8, 64, 32
ROWS = 11264
OWN = 1408
BLK = 1024
NBLK = ROWS // BLK
TBLK = 352
HALF = DH // 2

PLANE = [(dx, dy) for dx in range(4) for dy in range(4)]
Z_NEAR = (1, -1, 2, -2)
Z_FAR = ((-2, 1, (0, HALF)), (2, -1, (0, HALF)), (-2, 2, (0, HALF // 2)), (2, -2, (HALF // 2, HALF // 2)))


def contract_lanes(a, b, precision=None):
    return lax.dot_general(
        a, b, (((1,), (1,)), ((), ())), preferred_element_type=F32, precision=precision
    )


def softmax_weights(logits, temperature_logit):
    soft = jnp.maximum(temperature_logit, 0.0) + jnp.log(1.0 + jnp.exp(-jnp.abs(temperature_logit)))
    scaled = logits * (1.0 / (0.5 + soft))
    e = jnp.exp(scaled - jnp.max(scaled, axis=0, keepdims=True))
    return (e * (1.0 / jnp.sum(e, axis=0, keepdims=True))).astype(BF16)


def kernel(
    x_hbm, entry_hbm, part_hbm, sharp_hbm, qkv_hbm, exit_hbm, wide_hbm, narrow_hbm,
    out_ref,
    xv, eh, part_ref, sharp_ref, qkv_ref, waug, pT, cs, f0, f1, acc, wall, nown, wT, wn, mbuf, yall, m0, m1, n0, n1,
    pair, plane, zbuf,
    x_sem, in_sem, own_sem, far_sem, d2d_sem, pair_sem, plane_sem, z_sem,
):
    pts, z = lax.axis_index("pts"), lax.axis_index("wid")
    core = lax.rem(pts, 2)
    gx, gy = pts // 8, lax.rem(pts // 2, 4)
    partner = pts + 1 - 2 * core

    def pts_at(dx, dy):
        return (lax.rem(gx + dx, 4) * 4 + lax.rem(gy + dy, 4)) * 2 + core

    def z_at(dz):
        return lax.rem(z + dz + H, H)

    def x_copy(i):
        return pltpu.make_async_copy(
            x_hbm.at[pl.ds(i * BLK, BLK)], xv.at[pl.ds(i * BLK, BLK)], x_sem.at[i]
        )

    entry_copy = pltpu.make_async_copy(entry_hbm, eh, in_sem.at[0])
    small_copies = [
        pltpu.make_async_copy(part_hbm, part_ref, in_sem.at[9]),
        pltpu.make_async_copy(sharp_hbm, sharp_ref, in_sem.at[10]),
    ]
    qkv_copy = pltpu.make_async_copy(qkv_hbm, qkv_ref, in_sem.at[11])
    entry_copy.start()
    for copy in small_copies:
        copy.start()
    x_copy(0).start()
    own_copies = []
    for k, ref in enumerate((entry_hbm, exit_hbm, wide_hbm, narrow_hbm)):
        for c in range(2):
            own_copies.append(
                pltpu.make_async_copy(
                    ref.at[pl.ds(c * HALF, HALF)], wall.at[k, z, c], in_sem.at[1 + 2 * k + c]
                )
            )

    barrier = pltpu.get_barrier_semaphore()
    pl.semaphore_signal(barrier, inc=1, device_id=(partner, z), device_id_type=MESH)
    for dx, dy in PLANE[1:]:
        pl.semaphore_signal(barrier, inc=1, device_id=(pts_at(dx, dy), z), device_id_type=MESH)
    for dz in range(1, H):
        pl.semaphore_signal(barrier, inc=1, device_id=(pts, z_at(dz)), device_id_type=MESH)

    for copy in small_copies:
        copy.wait()
    sharp = jnp.broadcast_to(sharp_ref[...], (16, DH))
    sharp_hi = sharp.astype(BF16).astype(F32)
    row16 = lax.broadcasted_iota(jnp.int32, (16, DH), 0)
    tail = jnp.where(row16 == 0, sharp_hi, jnp.where(row16 == 1, sharp - sharp_hi, 0.0))
    table = jnp.concatenate([part_ref[...].astype(F32), tail], axis=0)
    pT[...] = jnp.concatenate([table, jnp.zeros((G + 16, DH), F32)], axis=1).astype(BF16)
    acc[...] = jnp.zeros_like(acc)
    one_at_64 = (lax.broadcasted_iota(jnp.int32, (1, 128), 1) == DH).astype(F32)

    entry_copy.wait()
    for i in range(1, NBLK):
        x_copy(i).start()
    for copy in own_copies:
        copy.start()
    qkv_copy.start()
    head = jnp.concatenate([eh[...].astype(F32), jnp.zeros((DH, D), F32)], axis=0).T
    cs[...] = jnp.sum(head, axis=0, keepdims=True)
    waug[:, 0:128] = head.astype(BF16)
    waug[:, 128:256] = jnp.full((D, 128), 1.0 / D, BF16)

    mats = (pl.ds(0, 1), pl.ds(1, 3))

    def to(ref, sems, device, target=None):
        return pltpu.make_async_remote_copy(
            src_ref=ref, dst_ref=ref if target is None else target, send_sem=sems.at[0], recv_sem=sems.at[1],
            device_id=device, device_id_type=MESH,
        )

    def half_of(g, offset, half, rows=pl.ds(0, HALF)):
        return wall.at[mats[g], z_at(offset), half, rows]

    def of_size(g, n, sems):
        return to(wall.at[mats[g], pl.ds(0, n), 0], sems.at[g], (partner, z))

    def weights_start():
        for copy in own_copies:
            copy.wait()
        for g in range(2):
            for dz in Z_NEAR:
                to(half_of(g, 0, core), own_sem.at[g], (pts, z_at(dz))).start()

    def weights_onward(g):
        of_size(g, 4, own_sem).wait_recv()
        for source, dz, rows in Z_FAR:
            to(half_of(g, source, core, pl.ds(*rows)), far_sem.at[g], (pts, z_at(dz))).start()
        for offset in Z_NEAR:
            to(half_of(g, offset, core), d2d_sem.at[g], (partner, z)).start()

    def weights_far(g):
        of_size(g, 3, far_sem).wait_recv()
        for offset in (3, -3, 4):
            to(half_of(g, offset, core), d2d_sem.at[g], (partner, z)).start()

    def weights_done(g):
        of_size(g, 7, d2d_sem).wait_recv()

    def project(i, fbuf):
        xb = xv[pl.ds(pl.multiple_of(i * BLK, BLK), BLK), :]
        y = jnp.dot(xb, waug[...], preferred_element_type=F32)
        xf = xb.astype(F32)
        sq = xf * xf
        sq = (sq[:, 0:128] + sq[:, 128:256]) + (sq[:, 256:384] + sq[:, 384:512])
        mean = y[:, 128:256]
        var = jnp.maximum(jnp.sum(sq, axis=1, keepdims=True) * (1.0 / D) - mean * mean, 0.0)
        feats = (y[:, 0:128] - cs[...] * mean) * lax.rsqrt(var + 1e-05)
        fbuf[...] = (feats + one_at_64).astype(BF16)

    def slices(fbuf):
        feats = fbuf[...]
        logits = contract_lanes(pT[...], feats)
        w = softmax_weights(logits[0:G], logits[G : G + 1] + logits[G + 1 : G + 2])
        acc[...] += jnp.dot(w, feats, preferred_element_type=F32)

    x_copy(0).wait()
    project(0, f0)

    def two_blocks(j, _):
        @pl.when(j == 1)
        def _():
            pl.semaphore_wait(barrier, 1 + 15 + 7)
            weights_start()

        x_copy(2 * j + 1).wait()
        x_copy(2 * j + 2).wait()
        slices(f0)
        project(2 * j + 1, f1)
        slices(f1)
        project(2 * j + 2, f0)
        return 0

    lax.fori_loop(0, NBLK // 2, two_blocks, 0)
    slices(f0)

    pair[0] = acc[...]
    pair_copy = to(pair.at[0], pair_sem, (partner, z), pair.at[1])
    pair_copy.start()
    weights_onward(0)
    pair_copy.wait_recv()
    plane[0] = pair[0] + pair[1]
    for r in range(1, 16):
        to(plane.at[0], plane_sem, (pts_at(*PLANE[r]), z), plane.at[r]).start()
    plane_all = to(plane.at[pl.ds(1, 15)], plane_sem, (partner, z))

    own = pl.multiple_of(z * OWN, 128)

    def own_norm(t, _):
        rows = xv[pl.ds(pl.multiple_of(own + t * TBLK, 32), TBLK), :].astype(F32)
        centred = rows - jnp.mean(rows, axis=1, keepdims=True)
        var = jnp.mean(centred * centred, axis=1, keepdims=True)
        nown[pl.ds(pl.multiple_of(t * TBLK, 32), TBLK), :] = (centred * lax.rsqrt(var + 1e-05)).astype(BF16)
        return 0

    lax.fori_loop(0, OWN // TBLK, own_norm, 0)
    weights_onward(1)
    weights_far(0)
    weights_done(0)
    yall[...] = contract_lanes(wall[0].reshape(D, D), nown[...]).astype(BF16)

    qkv_copy.wait()
    plane_all.wait_recv()
    sums = jnp.sum(plane[...], axis=0)
    tokens = sums[:, 0:DH] / (sums[:, DH : DH + 1] + 1e-05)
    queries = jnp.dot(tokens, qkv_ref[0], preferred_element_type=F32, precision=HIGH)
    keys = jnp.dot(tokens, qkv_ref[1], preferred_element_type=F32, precision=HIGH)
    values = jnp.dot(
        tokens, jnp.concatenate([qkv_ref[2], jnp.zeros((DH, DH), F32)], axis=1),
        preferred_element_type=F32, precision=HIGH,
    )
    scores = contract_lanes(queries, keys, precision=HIGH) * 0.125
    e = jnp.exp(scores - jnp.max(scores, axis=1, keepdims=True))
    attend = e / jnp.sum(e, axis=1, keepdims=True)
    zbuf[z] = jnp.dot(attend, values, preferred_element_type=F32, precision=HIGH).astype(BF16)

    for dz in range(1, H):
        to(zbuf.at[z], z_sem, (pts, z_at(dz))).start()
    z_all = to(zbuf.at[pl.ds(0, H - 1)], z_sem, (partner, z))

    for h in range(H):
        if h == H // 2:
            weights_far(1)
        logits = jnp.dot(pT[:, 0:DH], yall[h * DH : (h + 1) * DH, :], preferred_element_type=F32)
        wT[h * G : (h + 1) * G, :] = softmax_weights(
            logits[0:G], logits[G : G + 1] + logits[G + 1 : G + 2]
        )
    wn[...] = wT[...].T
    weights_done(1)
    z_all.wait_recv()

    for h in range(H):
        mbuf[h * G : (h + 1) * G, :] = jnp.dot(
            zbuf[h][:, 0:DH], wall[1, h].reshape(DH, D), preferred_element_type=F32
        ).astype(BF16)

    def mix(t, mid, normed):
        x_rows = xv[pl.ds(pl.multiple_of(own + t * TBLK, 32), TBLK), :].astype(F32)
        midway = x_rows + jnp.dot(wn[t * TBLK : (t + 1) * TBLK, :], mbuf[...], preferred_element_type=F32)
        centred = midway - jnp.mean(midway, axis=1, keepdims=True)
        var = jnp.mean(centred * centred, axis=1, keepdims=True)
        mid[...] = midway
        normed[...] = (centred * lax.rsqrt(var + 1e-05)).astype(BF16)

    def feed(t, mid, normed):
        hidden = jnp.dot(normed[...], wall[2].reshape(D, D), preferred_element_type=F32)
        hidden = jax.nn.gelu(hidden).astype(BF16)
        out = mid[...] + jnp.dot(hidden, wall[3].reshape(D, D), preferred_element_type=F32)
        out_ref[t * TBLK : (t + 1) * TBLK, :] = out.astype(BF16)

    stage = ((m0, n0), (m1, n1))
    mix(0, *stage[0])
    for t in range(OWN // TBLK):
        if t + 1 < OWN // TBLK:
            mix(t + 1, *stage[(t + 1) % 2])
        feed(t, *stage[t % 2])

    for g in range(2):
        of_size(g, 4, own_sem).wait_send()
        of_size(g, 3, far_sem).wait_send()
        of_size(g, 7, d2d_sem).wait_send()
    pair_copy.wait_send()
    plane_all.wait_send()
    z_all.wait_send()


OUT = pltpu.VMEM((OWN, D), BF16)


def local(x, entry, partition, sharpness, qkv, exit_matrix, widening, narrowing):
    hbm = pl.BlockSpec(memory_space=pl.ANY)
    vmem = pl.BlockSpec(memory_space=pltpu.VMEM)
    dma = pltpu.SemaphoreType.DMA
    return pl.pallas_call(
        kernel,
        out_shape=OUT,
        in_specs=[hbm] * 8,
        out_specs=vmem,
        scratch_shapes=[
            pltpu.VMEM((ROWS, D), BF16),
            pltpu.VMEM((DH, D), BF16),
            pltpu.VMEM((G, DH), BF16),
            pltpu.VMEM((1, DH), F32),
            pltpu.VMEM((3, DH, DH), F32),
            pltpu.VMEM((D, 256), BF16),
            pltpu.VMEM((G + 16, 128), BF16),
            pltpu.VMEM((1, 128), F32),
            pltpu.VMEM((BLK, 128), BF16),
            pltpu.VMEM((BLK, 128), BF16),
            pltpu.VMEM((G, 128), F32),
            pltpu.VMEM((4, H, 2, HALF, D), BF16),
            pltpu.VMEM((OWN, D), BF16),
            pltpu.VMEM((H * G, OWN), BF16),
            pltpu.VMEM((OWN, H * G), BF16),
            pltpu.VMEM((H * G, D), BF16),
            pltpu.VMEM((D, OWN), BF16),
            pltpu.VMEM((TBLK, D), F32),
            pltpu.VMEM((TBLK, D), F32),
            pltpu.VMEM((TBLK, D), BF16),
            pltpu.VMEM((TBLK, D), BF16),
            pltpu.VMEM((2, G, 128), F32),
            pltpu.VMEM((16, G, 128), F32),
            pltpu.VMEM((H, G, 128), BF16),
            dma((NBLK,)),
            dma((12,)),
            dma((2, 2)),
            dma((2, 2)),
            dma((2, 2)),
            dma((2,)),
            dma((2,)),
            dma((2,)),
        ],
        compiler_params=pltpu.CompilerParams(
            collective_id=0, has_side_effects=True, vmem_limit_bytes=60 * 2**20
        ),
    )(x, entry.T, partition.T, sharpness.reshape(1, DH), qkv, exit_matrix, widening, narrowing)


def solution(mesh):
    placed = (
        P("pts", None), P(None, "wid"), P(), P(), P(),
        P("wid", None), P("wid", None), P("wid", None),
    )
    return jax.shard_map(
        local, mesh=mesh, in_specs=placed, out_specs=P(("pts", "wid"), None), check_vma=False
    )
```

```python
import functools

import jax
import jax.numpy as jnp
from jax import lax
from jax.experimental import pallas as pl
from jax.experimental.pallas import tpu as pltpu
from jax.sharding import PartitionSpec as P

MESH = pl.DeviceIdType.MESH
F32, BF16 = jnp.float32, jnp.bfloat16
HIGH = lax.Precision.HIGHEST

D, H, DH, G = 512, 8, 64, 32
ROWS = 11264
OWN = 1408
BLK = 1408
SUB = 352
NBLK = ROWS // BLK
TBLK = 352
HALF = DH // 2

PLANE = [(dx, dy) for dx in range(4) for dy in range(4)]
Z_NEAR = (1, -1, 2, -2)
Z_FAR = ((-2, 1, (0, HALF)), (2, -1, (0, HALF)), (-2, 2, (0, HALF // 2)), (2, -2, (HALF // 2, HALF // 2)))


def contract_lanes(a, b, precision=None):
    return lax.dot_general(
        a, b, (((1,), (1,)), ((), ())), preferred_element_type=F32, precision=precision
    )


def inverse_temperature(logit):
    return 1.0 / (0.5 + jnp.maximum(logit, 0.0) + jnp.log(1.0 + jnp.exp(-jnp.abs(logit))))


def softmax_weights(logits):
    scaled = logits[0:G] * inverse_temperature(logits[G : G + 1] + logits[G + 1 : G + 2])
    e = jnp.exp(scaled - jnp.max(scaled, axis=0, keepdims=True))
    return (e * (1.0 / jnp.sum(e, axis=0, keepdims=True))).astype(BF16)


def kernel(
    x_hbm, entry_hbm, part_hbm, sharp_hbm, qkv_hbm, exit_hbm, wide_hbm, narrow_hbm,
    out_ref,
    xv, eh, part_ref, sharp_ref, qkv_ref, waug, pT, cs, f0, f1, acc, wall, nown, wT, wn, mbuf, yall, m0, m1, n0, n1,
    pair, plane, zbuf,
    x_sem, in_sem, own_sem, far_sem, d2d_sem, pair_sem, plane_sem, z_sem,
):
    pts, z = lax.axis_index("pts"), lax.axis_index("wid")
    core = lax.rem(pts, 2)
    gx, gy = pts // 8, lax.rem(pts // 2, 4)
    partner = pts + 1 - 2 * core

    def pts_at(dx, dy):
        return (lax.rem(gx + dx, 4) * 4 + lax.rem(gy + dy, 4)) * 2 + core

    def z_at(dz):
        return lax.rem(z + dz + H, H)

    def x_copy(i):
        return pltpu.make_async_copy(
            x_hbm.at[pl.ds(i * BLK, BLK)], xv.at[pl.ds(i * BLK, BLK)], x_sem.at[i]
        )

    entry_copy = pltpu.make_async_copy(entry_hbm, eh, in_sem.at[0])
    small_copies = [
        pltpu.make_async_copy(part_hbm, part_ref, in_sem.at[9]),
        pltpu.make_async_copy(sharp_hbm, sharp_ref, in_sem.at[10]),
    ]
    qkv_copy = pltpu.make_async_copy(qkv_hbm, qkv_ref, in_sem.at[11])
    entry_copy.start()
    for copy in small_copies:
        copy.start()
    x_copy(0).start()
    own_copies = []
    for k, ref in enumerate((entry_hbm, exit_hbm, wide_hbm, narrow_hbm)):
        for c in range(2):
            own_copies.append(
                pltpu.make_async_copy(
                    ref.at[pl.ds(c * HALF, HALF)], wall.at[k, z, c], in_sem.at[1 + 2 * k + c]
                )
            )

    barrier = pltpu.get_barrier_semaphore()
    pl.semaphore_signal(barrier, inc=1, device_id=(partner, z), device_id_type=MESH)
    for dx, dy in PLANE[1:]:
        pl.semaphore_signal(barrier, inc=1, device_id=(pts_at(dx, dy), z), device_id_type=MESH)
    for dz in range(1, H):
        pl.semaphore_signal(barrier, inc=1, device_id=(pts, z_at(dz)), device_id_type=MESH)

    for copy in small_copies:
        copy.wait()
    sharp = jnp.broadcast_to(sharp_ref[...], (16, DH))
    sharp_hi = sharp.astype(BF16).astype(F32)
    row16 = lax.broadcasted_iota(jnp.int32, (16, DH), 0)
    tail = jnp.where(row16 == 0, sharp_hi, jnp.where(row16 == 1, sharp - sharp_hi, 0.0))
    table = jnp.concatenate([part_ref[...].astype(F32), tail], axis=0)
    pT[...] = jnp.concatenate([table, jnp.zeros((G + 16, DH), F32)], axis=1).astype(BF16)
    acc[...] = jnp.zeros_like(acc)
    one_at_64 = (lax.broadcasted_iota(jnp.int32, (1, 128), 1) == DH).astype(F32)

    entry_copy.wait()
    for i in range(1, NBLK):
        x_copy(i).start()
    for copy in own_copies:
        copy.start()
    qkv_copy.start()
    head = jnp.concatenate([eh[...].astype(F32), jnp.zeros((DH, D), F32)], axis=0).T
    cs[...] = jnp.sum(head, axis=0, keepdims=True)
    waug[:, 0:128] = head.astype(BF16)
    waug[:, 128:256] = jnp.full((D, 128), 1.0 / D, BF16)

    mats = (pl.ds(0, 1), pl.ds(1, 3))

    def to(ref, sems, device, target=None):
        return pltpu.make_async_remote_copy(
            src_ref=ref, dst_ref=ref if target is None else target, send_sem=sems.at[0], recv_sem=sems.at[1],
            device_id=device, device_id_type=MESH,
        )

    def half_of(g, offset, half, rows=pl.ds(0, HALF)):
        return wall.at[mats[g], z_at(offset), half, rows]

    def of_size(g, n, sems):
        return to(wall.at[mats[g], pl.ds(0, n), 0], sems.at[g], (partner, z))

    def weights_start():
        for copy in own_copies:
            copy.wait()
        for g in range(2):
            for dz in Z_NEAR:
                to(half_of(g, 0, core), own_sem.at[g], (pts, z_at(dz))).start()

    def weights_onward(g):
        of_size(g, 4, own_sem).wait_recv()
        for source, dz, rows in Z_FAR:
            to(half_of(g, source, core, pl.ds(*rows)), far_sem.at[g], (pts, z_at(dz))).start()
        for offset in Z_NEAR:
            to(half_of(g, offset, core), d2d_sem.at[g], (partner, z)).start()

    def weights_far(g):
        of_size(g, 3, far_sem).wait_recv()
        for offset in (3, -3, 4):
            to(half_of(g, offset, core), d2d_sem.at[g], (partner, z)).start()

    def weights_done(g):
        of_size(g, 7, d2d_sem).wait_recv()

    def project(i, q, fbuf):
        start = i * BLK + q * SUB
        if not isinstance(start, int):
            start = pl.multiple_of(start, SUB)
        xb = xv[pl.ds(start, SUB), :]
        y = jnp.dot(xb, waug[...], preferred_element_type=F32)
        xf = xb.astype(F32)
        sq = xf * xf
        sq = (sq[:, 0:128] + sq[:, 128:256]) + (sq[:, 256:384] + sq[:, 384:512])
        mean = y[:, 128:256]
        var = jnp.maximum(jnp.sum(sq, axis=1, keepdims=True) * (1.0 / D) - mean * mean, 0.0)
        feats = (y[:, 0:128] - cs[...] * mean) * lax.rsqrt(var + 1e-05)
        fbuf[q * SUB : (q + 1) * SUB, :] = (feats + one_at_64).astype(BF16)

    def slices(fbuf):
        logits = contract_lanes(pT[...], fbuf[...])
        yield
        scaled = logits[0:G] * inverse_temperature(logits[G : G + 1] + logits[G + 1 : G + 2])
        e = jnp.exp(scaled - jnp.max(scaled, axis=0, keepdims=True))
        yield
        w = (e * (1.0 / jnp.sum(e, axis=0, keepdims=True))).astype(BF16)
        yield
        acc[...] += jnp.dot(w, fbuf[...], preferred_element_type=F32)
        yield

    def project_and_slices(i, fbuf, other):
        steps = slices(other)
        for q in range(BLK // SUB):
            project(i, q, fbuf)
            next(steps)

    x_copy(0).wait()
    for q in range(BLK // SUB):
        project(0, q, f0)

    def two_blocks(j, _):
        @pl.when(j == 1)
        def _():
            pl.semaphore_wait(barrier, 1 + 15 + 7)
            weights_start()

        x_copy(2 * j + 1).wait()
        x_copy(2 * j + 2).wait()
        project_and_slices(2 * j + 1, f1, f0)
        project_and_slices(2 * j + 2, f0, f1)
        return 0

    lax.fori_loop(0, NBLK // 2 - 1, two_blocks, 0)
    x_copy(NBLK - 1).wait()
    project_and_slices(NBLK - 1, f1, f0)
    for _ in slices(f1):
        pass

    pair[0] = acc[...]
    pair_copy = to(pair.at[0], pair_sem, (partner, z), pair.at[1])
    pair_copy.start()
    weights_onward(0)
    pair_copy.wait_recv()
    plane[0] = pair[0] + pair[1]
    for r in range(1, 16):
        to(plane.at[0], plane_sem, (pts_at(*PLANE[r]), z), plane.at[r]).start()
    plane_all = to(plane.at[pl.ds(1, 15)], plane_sem, (partner, z))

    own = pl.multiple_of(z * OWN, 128)

    def own_norm(t, _):
        rows = xv[pl.ds(pl.multiple_of(own + t * TBLK, 32), TBLK), :].astype(F32)
        centred = rows - jnp.mean(rows, axis=1, keepdims=True)
        var = jnp.mean(centred * centred, axis=1, keepdims=True)
        nown[pl.ds(pl.multiple_of(t * TBLK, 32), TBLK), :] = (centred * lax.rsqrt(var + 1e-05)).astype(BF16)
        return 0

    lax.fori_loop(0, OWN // TBLK, own_norm, 0)
    weights_onward(1)
    weights_far(0)

    qkv_copy.wait()
    plane_all.wait_recv()
    sums = jnp.sum(plane[...], axis=0)
    tokens = sums[:, 0:DH] / (sums[:, DH : DH + 1] + 1e-05)
    queries = jnp.dot(tokens, qkv_ref[0], preferred_element_type=F32, precision=HIGH)
    keys = jnp.dot(tokens, qkv_ref[1], preferred_element_type=F32, precision=HIGH)
    values = jnp.dot(
        tokens, jnp.concatenate([qkv_ref[2], jnp.zeros((DH, DH), F32)], axis=1),
        preferred_element_type=F32, precision=HIGH,
    )
    scores = contract_lanes(queries, keys, precision=HIGH) * 0.125
    e = jnp.exp(scores - jnp.max(scores, axis=1, keepdims=True))
    attend = e / jnp.sum(e, axis=1, keepdims=True)
    zbuf[z] = jnp.dot(attend, values, preferred_element_type=F32, precision=HIGH).astype(BF16)

    for dz in range(1, H):
        to(zbuf.at[z], z_sem, (pts, z_at(dz))).start()
    z_all = to(zbuf.at[pl.ds(0, H - 1)], z_sem, (partner, z))

    weights_done(0)
    yall[...] = contract_lanes(wall[0].reshape(D, D), nown[...]).astype(BF16)
    for h in range(H):
        if h == H // 2:
            weights_far(1)
        logits = jnp.dot(pT[:, 0:DH], yall[h * DH : (h + 1) * DH, :], preferred_element_type=F32)
        wT[h * G : (h + 1) * G, :] = softmax_weights(logits)
    wn[...] = wT[...].T
    weights_done(1)
    z_all.wait_recv()

    for h in range(H):
        mbuf[h * G : (h + 1) * G, :] = jnp.dot(
            zbuf[h][:, 0:DH], wall[1, h].reshape(DH, D), preferred_element_type=F32
        ).astype(BF16)

    def mix(t, mid, normed):
        x_rows = xv[pl.ds(pl.multiple_of(own + t * TBLK, 32), TBLK), :].astype(F32)
        midway = x_rows + jnp.dot(wn[t * TBLK : (t + 1) * TBLK, :], mbuf[...], preferred_element_type=F32)
        centred = midway - jnp.mean(midway, axis=1, keepdims=True)
        var = jnp.mean(centred * centred, axis=1, keepdims=True)
        mid[...] = midway
        normed[...] = (centred * lax.rsqrt(var + 1e-05)).astype(BF16)

    def feed(t, mid, normed):
        hidden = jnp.dot(normed[...], wall[2].reshape(D, D), preferred_element_type=F32)
        hidden = jax.nn.gelu(hidden).astype(BF16)
        out = mid[...] + jnp.dot(hidden, wall[3].reshape(D, D), preferred_element_type=F32)
        out_ref[t * TBLK : (t + 1) * TBLK, :] = out.astype(BF16)

    stage = ((m0, n0), (m1, n1))
    mix(0, *stage[0])
    for t in range(OWN // TBLK):
        if t + 1 < OWN // TBLK:
            mix(t + 1, *stage[(t + 1) % 2])
        feed(t, *stage[t % 2])

    for g in range(2):
        of_size(g, 4, own_sem).wait_send()
        of_size(g, 3, far_sem).wait_send()
        of_size(g, 7, d2d_sem).wait_send()
    pair_copy.wait_send()
    plane_all.wait_send()
    z_all.wait_send()


OUT = pltpu.VMEM((OWN, D), BF16)


def local(x, entry, partition, sharpness, qkv, exit_matrix, widening, narrowing):
    hbm = pl.BlockSpec(memory_space=pl.ANY)
    vmem = pl.BlockSpec(memory_space=pltpu.VMEM)
    dma = pltpu.SemaphoreType.DMA
    return pl.pallas_call(
        kernel,
        out_shape=OUT,
        in_specs=[hbm] * 8,
        out_specs=vmem,
        scratch_shapes=[
            pltpu.VMEM((ROWS, D), BF16),
            pltpu.VMEM((DH, D), BF16),
            pltpu.VMEM((G, DH), BF16),
            pltpu.VMEM((1, DH), F32),
            pltpu.VMEM((3, DH, DH), F32),
            pltpu.VMEM((D, 256), BF16),
            pltpu.VMEM((G + 16, 128), BF16),
            pltpu.VMEM((1, 128), F32),
            pltpu.VMEM((BLK, 128), BF16),
            pltpu.VMEM((BLK, 128), BF16),
            pltpu.VMEM((G, 128), F32),
            pltpu.VMEM((4, H, 2, HALF, D), BF16),
            pltpu.VMEM((OWN, D), BF16),
            pltpu.VMEM((H * G, OWN), BF16),
            pltpu.VMEM((OWN, H * G), BF16),
            pltpu.VMEM((H * G, D), BF16),
            pltpu.VMEM((D, OWN), BF16),
            pltpu.VMEM((TBLK, D), F32),
            pltpu.VMEM((TBLK, D), F32),
            pltpu.VMEM((TBLK, D), BF16),
            pltpu.VMEM((TBLK, D), BF16),
            pltpu.VMEM((2, G, 128), F32),
            pltpu.VMEM((16, G, 128), F32),
            pltpu.VMEM((H, G, 128), BF16),
            dma((NBLK,)),
            dma((12,)),
            dma((2, 2)),
            dma((2, 2)),
            dma((2, 2)),
            dma((2,)),
            dma((2,)),
            dma((2,)),
        ],
        compiler_params=pltpu.CompilerParams(
            collective_id=0, has_side_effects=True, vmem_limit_bytes=60 * 2**20
        ),
    )(x, entry.T, partition.T, sharpness.reshape(1, DH), qkv, exit_matrix, widening, narrowing)


def solution(mesh):
    placed = (
        P("pts", None), P(None, "wid"), P(), P(), P(),
        P("wid", None), P("wid", None), P("wid", None),
    )
    return jax.shard_map(
        local, mesh=mesh, in_specs=placed, out_specs=P(("pts", "wid"), None), check_vma=False
    )
```

```python
import functools

import jax
import jax.numpy as jnp
from jax import lax
from jax.experimental import pallas as pl
from jax.experimental.pallas import tpu as pltpu
from jax.sharding import PartitionSpec as P

MESH = pl.DeviceIdType.MESH
F32, BF16 = jnp.float32, jnp.bfloat16
HIGH = lax.Precision.HIGHEST

D, H, DH, G = 512, 8, 64, 32
ROWS = 11264
OWN = 1408
BLK = 1408
PAIRS = BLK // 2
DOT = 352
SUB = 176
NBLK = ROWS // BLK
NORM_ROWS = 352
TBLK = 704
HALF = DH // 2

PLANE = [(dx, dy) for dx in range(4) for dy in range(4)]


def contract_lanes(a, b, precision=None):
    return lax.dot_general(
        a, b, (((1,), (1,)), ((), ())), preferred_element_type=F32, precision=precision
    )


def inverse_temperature(logit):
    return 1.0 / (0.5 + jnp.maximum(logit, 0.0) + jnp.log(1.0 + jnp.exp(-jnp.abs(logit))))


def softmax_weights(logits):
    scaled = logits[0:G] * inverse_temperature(logits[G : G + 1] + logits[G + 1 : G + 2])
    e = jnp.exp(scaled - jnp.max(scaled, axis=0, keepdims=True))
    return (e * (1.0 / jnp.sum(e, axis=0, keepdims=True))).astype(BF16)


def kernel(
    x_hbm, entry_hbm, part_hbm, sharp_hbm, qkv_hbm, exit_hbm, wide_hbm, narrow_hbm,
    out_ref,
    xv, eh, part_ref, sharp_ref, qkv_ref, waug, pT, cs, f0, f1, acc, wall, nown, wT, wn, mbuf, yall, m0, m1, n0, n1,
    pair, plane, zbuf,
    x_sem, in_sem, own_sem, hop_sem, far_sem, d2d_sem, pair_sem, plane_sem, z_sem,
):
    pts, z = lax.axis_index("pts"), lax.axis_index("wid")
    core = lax.rem(pts, 2)
    gx, gy = pts // 8, lax.rem(pts // 2, 4)
    partner = pts + 1 - 2 * core

    def pts_at(dx, dy):
        return (lax.rem(gx + dx, 4) * 4 + lax.rem(gy + dy, 4)) * 2 + core

    def z_at(dz):
        return lax.rem(z + dz + H, H)

    def x_copy(i):
        return pltpu.make_async_copy(
            x_hbm.at[pl.ds(i * BLK, BLK)], xv.at[pl.ds(i * BLK, BLK)], x_sem.at[i]
        )

    entry_copy = pltpu.make_async_copy(entry_hbm, eh, in_sem.at[0])
    small_copies = [
        pltpu.make_async_copy(part_hbm, part_ref, in_sem.at[9]),
        pltpu.make_async_copy(sharp_hbm, sharp_ref, in_sem.at[10]),
    ]
    qkv_copy = pltpu.make_async_copy(qkv_hbm, qkv_ref, in_sem.at[11])
    entry_copy.start()
    for copy in small_copies:
        copy.start()
    x_copy(0).start()
    own_copies = []
    for k, ref in enumerate((entry_hbm, exit_hbm, wide_hbm, narrow_hbm)):
        for c in range(2):
            own_copies.append(
                pltpu.make_async_copy(
                    ref.at[pl.ds(c * HALF, HALF)], wall.at[k, z, c], in_sem.at[1 + 2 * k + c]
                )
            )

    for copy in own_copies:
        copy.start()
    qkv_copy.start()

    barrier = pltpu.get_barrier_semaphore()
    pl.semaphore_signal(barrier, inc=1, device_id=(partner, z), device_id_type=MESH)
    for dx, dy in PLANE[1:]:
        pl.semaphore_signal(barrier, inc=1, device_id=(pts_at(dx, dy), z), device_id_type=MESH)
    for dz in range(1, H):
        pl.semaphore_signal(barrier, inc=1, device_id=(pts, z_at(dz)), device_id_type=MESH)

    for copy in small_copies:
        copy.wait()
    sharp = jnp.broadcast_to(sharp_ref[...], (16, DH))
    sharp_hi = sharp.astype(BF16).astype(F32)
    row16 = lax.broadcasted_iota(jnp.int32, (16, DH), 0)
    tail = jnp.where(row16 == 0, sharp_hi, jnp.where(row16 == 1, sharp - sharp_hi, 0.0))
    table = jnp.concatenate([part_ref[...].astype(F32), tail], axis=0)
    blank = jnp.zeros((G + 16, DH), F32)
    pT[0 : G + 16, :] = jnp.concatenate([table, blank], axis=1).astype(BF16)
    pT[G + 16 :, :] = jnp.concatenate([blank, table], axis=1).astype(BF16)
    acc[...] = jnp.zeros_like(acc)

    for i in range(1, NBLK):
        x_copy(i).start()
    entry_copy.wait()
    head = eh[...].astype(F32)
    low = lax.broadcasted_iota(jnp.int32, (D, 128), 1) < DH
    both = jnp.concatenate([head, head], axis=0).T
    cs[...] = jnp.sum(both, axis=0, keepdims=True)
    for half, lanes in ((0, low), (1, jnp.logical_not(low))):
        waug[half * D : (half + 1) * D, 0:128] = jnp.where(lanes, both, 0.0).astype(BF16)
        waug[half * D : (half + 1) * D, 128:256] = jnp.where(lanes, 1.0 / D, 0.0).astype(BF16)

    def to(ref, sems, device, target=None):
        return pltpu.make_async_remote_copy(
            src_ref=ref, dst_ref=ref if target is None else target, send_sem=sems.at[0], recv_sem=sems.at[1],
            device_id=device, device_id_type=MESH,
        )

    def half_of(g, offset, half, rows=pl.ds(0, HALF)):
        return wall.at[g, z_at(offset), half, rows]

    def of_size(g, n, sems):
        return to(wall.at[g, pl.ds(0, n), 0], sems.at[g], (partner, z))

    def to_partner(g, offsets):
        for offset in offsets:
            to(half_of(g, offset, core), d2d_sem.at[g], (partner, z)).start()

    def weights_1():
        for copy in own_copies:
            copy.wait()
        for g in range(4):
            for d in (1, -1):
                to(half_of(g, 0, core), own_sem.at[g], (pts, z_at(d))).start()

    def weights_2(g):
        of_size(g, 2, own_sem).wait_recv()
        for d in (1, -1):
            to(half_of(g, -d, core), hop_sem.at[g], (pts, z_at(d))).start()

    def weights_3(g):
        of_size(g, 2, hop_sem).wait_recv()
        for d, first in ((1, 0), (-1, HALF // 2)):
            to(half_of(g, -2 * d, core), far_sem.at[g], (pts, z_at(d))).start()
            rows = pl.ds(first, HALF // 2)
            to(half_of(g, -2 * d, core, rows), far_sem.at[g], (pts, z_at(2 * d))).start()
        to_partner(g, (1, -1, 2, -2))

    def weights_far(g):
        of_size(g, 3, far_sem).wait_recv()
        to_partner(g, (3, -3, 4))

    def weights_done(g):
        of_size(g, 7, d2d_sem).wait_recv()

    def project(i, q, fbuf):
        start = i * BLK + q * DOT
        if not isinstance(start, int):
            start = pl.multiple_of(start, 32)
        first = xv[pl.ds(start, DOT), :]
        second = xv[pl.ds(start + PAIRS, DOT), :]
        y = jnp.dot(jnp.concatenate([first, second], axis=1), waug[...], preferred_element_type=F32)
        lower = lax.broadcasted_iota(jnp.int32, (SUB, 128), 1) < DH

        def square_sums(rows):
            sq = rows.astype(F32)
            sq = sq * sq
            sq = (sq[:, 0:128] + sq[:, 128:256]) + (sq[:, 256:384] + sq[:, 384:512])
            return jnp.sum(sq, axis=1, keepdims=True)

        for r in range(0, DOT, SUB):
            rows = slice(r, r + SUB)
            squares = jnp.where(lower, square_sums(first[rows]), square_sums(second[rows]))
            mean = y[rows, 128:256]
            var = jnp.maximum(squares * (1.0 / D) - mean * mean, 0.0)
            feats = (y[rows, 0:128] - cs[...] * mean) * lax.rsqrt(var + 1e-05)
            fbuf[q * DOT + r : q * DOT + r + SUB, :] = feats.astype(BF16)
            yield

    def slices(fbuf):
        logits = contract_lanes(pT[...], fbuf[...])
        yield
        exps = []
        for top in (0, G + 16):
            scaled = logits[top : top + G] * inverse_temperature(
                logits[top + G : top + G + 1] + logits[top + G + 1 : top + G + 2]
            )
            exps.append(jnp.exp(scaled - jnp.max(scaled, axis=0, keepdims=True)))
        yield
        w = [(e * (1.0 / jnp.sum(e, axis=0, keepdims=True))).astype(BF16) for e in exps]
        yield
        with_ones = jnp.concatenate([fbuf[...], jnp.ones((PAIRS, 128), BF16)], axis=1)
        acc[...] += jnp.dot(jnp.concatenate(w, axis=0), with_ones, preferred_element_type=F32)
        yield

    def project_and_slices(i, fbuf, other):
        steps = slices(other)
        for q in range(PAIRS // DOT):
            for _ in project(i, q, fbuf):
                next(steps)

    x_copy(0).wait()
    for q in range(PAIRS // DOT):
        for _ in project(0, q, f0):
            pass

    start_at = (z < 1).astype(jnp.int32) + (z < 4).astype(jnp.int32)

    def two_blocks(j, _):
        @pl.when(j == start_at)
        def _():
            pl.semaphore_wait(barrier, 1 + 15 + 7)
            weights_1()

        x_copy(2 * j + 1).wait()
        x_copy(2 * j + 2).wait()
        project_and_slices(2 * j + 1, f1, f0)
        project_and_slices(2 * j + 2, f0, f1)
        return 0

    lax.fori_loop(0, NBLK // 2 - 1, two_blocks, 0)
    weights_2(0)
    weights_2(1)
    x_copy(NBLK - 1).wait()
    project_and_slices(NBLK - 1, f1, f0)
    weights_2(2)
    weights_2(3)
    for _ in slices(f1):
        pass

    lane = lax.broadcasted_iota(jnp.int32, (G, 128), 1)
    numerator = acc[0:G, 0:128] + pltpu.roll(acc[G:, 0:128], DH, axis=1)
    pair[0] = jnp.where(lane < DH, numerator, acc[0:G, 128:256] + acc[G:, 128:256])
    pair_copy = to(pair.at[0], pair_sem, (partner, z), pair.at[1])
    pair_copy.start()
    pair_copy.wait_recv()
    plane[0] = pair[0] + pair[1]
    for r in range(1, 16):
        to(plane.at[0], plane_sem, (pts_at(*PLANE[r]), z), plane.at[r]).start()
    plane_all = to(plane.at[pl.ds(1, 15)], plane_sem, (partner, z))

    weights_3(0)
    own = pl.multiple_of(z * OWN, 128)

    def own_norm(t, _):
        rows = xv[pl.ds(pl.multiple_of(own + t * NORM_ROWS, 32), NORM_ROWS), :].astype(F32)
        centred = rows - jnp.mean(rows, axis=1, keepdims=True)
        var = jnp.mean(centred * centred, axis=1, keepdims=True)
        nown[pl.ds(pl.multiple_of(t * NORM_ROWS, 32), NORM_ROWS), :] = (centred * lax.rsqrt(var + 1e-05)).astype(BF16)
        return 0

    lax.fori_loop(0, OWN // NORM_ROWS, own_norm, 0)
    for g in range(1, 4):
        weights_3(g)
    weights_far(0)

    qkv_copy.wait()
    plane_all.wait_recv()
    sums = jnp.sum(plane[...], axis=0)
    tokens = sums[:, 0:DH] / (sums[:, DH : DH + 1] + 1e-05)
    queries = jnp.dot(tokens, qkv_ref[0], preferred_element_type=F32, precision=HIGH)
    keys = jnp.dot(tokens, qkv_ref[1], preferred_element_type=F32, precision=HIGH)
    values = jnp.dot(
        tokens, jnp.concatenate([qkv_ref[2], jnp.zeros((DH, DH), F32)], axis=1),
        preferred_element_type=F32, precision=HIGH,
    )
    scores = contract_lanes(queries, keys, precision=HIGH) * 0.125
    e = jnp.exp(scores - jnp.max(scores, axis=1, keepdims=True))
    attend = e / jnp.sum(e, axis=1, keepdims=True)
    zbuf[z] = jnp.dot(attend, values, preferred_element_type=F32, precision=HIGH).astype(BF16)

    for dz in range(1, H):
        to(zbuf.at[z], z_sem, (pts, z_at(dz))).start()
    z_all = to(zbuf.at[pl.ds(0, H - 1)], z_sem, (partner, z))

    weights_far(1)
    weights_done(0)
    yall[...] = contract_lanes(wall[0].reshape(D, D), nown[...]).astype(BF16)
    for h in range(H):
        if h == 2:
            weights_far(2)
        if h == 5:
            weights_far(3)
        logits = jnp.dot(pT[0 : G + 16, 0:DH], yall[h * DH : (h + 1) * DH, :], preferred_element_type=F32)
        wT[h * G : (h + 1) * G, :] = softmax_weights(logits)
    wn[...] = wT[...].T
    z_all.wait_recv()
    weights_done(1)

    for h in range(H):
        mbuf[h * G : (h + 1) * G, :] = jnp.dot(
            zbuf[h][:, 0:DH], wall[1, h].reshape(DH, D), preferred_element_type=F32
        ).astype(BF16)

    def mix(t, mid, normed):
        x_rows = xv[pl.ds(pl.multiple_of(own + t * TBLK, 32), TBLK), :].astype(F32)
        midway = x_rows + jnp.dot(wn[t * TBLK : (t + 1) * TBLK, :], mbuf[...], preferred_element_type=F32)
        centred = midway - jnp.mean(midway, axis=1, keepdims=True)
        var = jnp.mean(centred * centred, axis=1, keepdims=True)
        mid[...] = midway
        normed[...] = (centred * lax.rsqrt(var + 1e-05)).astype(BF16)

    def feed(t, mid, normed):
        hidden = jnp.dot(normed[...], wall[2].reshape(D, D), preferred_element_type=F32)
        hidden = jax.nn.gelu(hidden).astype(BF16)
        out = mid[...] + jnp.dot(hidden, wall[3].reshape(D, D), preferred_element_type=F32)
        out_ref[t * TBLK : (t + 1) * TBLK, :] = out.astype(BF16)

    stage = ((m0, n0), (m1, n1))
    mix(0, *stage[0])
    weights_done(2)
    weights_done(3)
    for t in range(OWN // TBLK):
        if t + 1 < OWN // TBLK:
            mix(t + 1, *stage[(t + 1) % 2])
        feed(t, *stage[t % 2])

    for g in range(4):
        of_size(g, 2, own_sem).wait_send()
        of_size(g, 2, hop_sem).wait_send()
        of_size(g, 3, far_sem).wait_send()
        of_size(g, 7, d2d_sem).wait_send()
    pair_copy.wait_send()
    plane_all.wait_send()
    z_all.wait_send()


OUT = pltpu.VMEM((OWN, D), BF16)


def local(x, entry, partition, sharpness, qkv, exit_matrix, widening, narrowing):
    hbm = pl.BlockSpec(memory_space=pl.ANY)
    vmem = pl.BlockSpec(memory_space=pltpu.VMEM)
    dma = pltpu.SemaphoreType.DMA
    return pl.pallas_call(
        kernel,
        out_shape=OUT,
        in_specs=[hbm] * 8,
        out_specs=vmem,
        scratch_shapes=[
            pltpu.VMEM((ROWS, D), BF16),
            pltpu.VMEM((DH, D), BF16),
            pltpu.VMEM((G, DH), BF16),
            pltpu.VMEM((1, DH), F32),
            pltpu.VMEM((3, DH, DH), F32),
            pltpu.VMEM((2 * D, 256), BF16),
            pltpu.VMEM((2 * (G + 16), 128), BF16),
            pltpu.VMEM((1, 128), F32),
            pltpu.VMEM((PAIRS, 128), BF16),
            pltpu.VMEM((PAIRS, 128), BF16),
            pltpu.VMEM((2 * G, 256), F32),
            pltpu.VMEM((4, H, 2, HALF, D), BF16),
            pltpu.VMEM((OWN, D), BF16),
            pltpu.VMEM((H * G, OWN), BF16),
            pltpu.VMEM((OWN, H * G), BF16),
            pltpu.VMEM((H * G, D), BF16),
            pltpu.VMEM((D, OWN), BF16),
            pltpu.VMEM((TBLK, D), F32),
            pltpu.VMEM((TBLK, D), F32),
            pltpu.VMEM((TBLK, D), BF16),
            pltpu.VMEM((TBLK, D), BF16),
            pltpu.VMEM((2, G, 128), F32),
            pltpu.VMEM((16, G, 128), F32),
            pltpu.VMEM((H, G, 128), BF16),
            dma((NBLK,)),
            dma((12,)),
            dma((4, 2)),
            dma((4, 2)),
            dma((4, 2)),
            dma((4, 2)),
            dma((2,)),
            dma((2,)),
            dma((2,)),
        ],
        compiler_params=pltpu.CompilerParams(
            collective_id=0, has_side_effects=True, vmem_limit_bytes=60 * 2**20
        ),
    )(x, entry.T, partition.T, sharpness.reshape(1, DH), qkv, exit_matrix, widening, narrowing)


def solution(mesh):
    placed = (
        P("pts", None), P(None, "wid"), P(), P(), P(),
        P("wid", None), P("wid", None), P("wid", None),
    )
    return jax.shard_map(
        local, mesh=mesh, in_specs=placed, out_specs=P(("pts", "wid"), None), check_vma=False
    )
```

```python
import functools

import jax
import jax.numpy as jnp
from jax import lax
from jax.experimental import pallas as pl
from jax.experimental.pallas import tpu as pltpu
from jax.sharding import PartitionSpec as P

MESH = pl.DeviceIdType.MESH
F32, BF16 = jnp.float32, jnp.bfloat16
HIGH = lax.Precision.HIGHEST

D, H, DH, G = 512, 8, 64, 32
ROWS = 11264
OWN = 1408
BLK = 1408
PAIRS = BLK // 2
DOT = 352
SUB = 176
NBLK = ROWS // BLK
NORM_ROWS = 352
TBLK = 704
HALF = DH // 2

PLANE = [(dx, dy) for dx in range(4) for dy in range(4)]


def contract_lanes(a, b, precision=None):
    return lax.dot_general(
        a, b, (((1,), (1,)), ((), ())), preferred_element_type=F32, precision=precision
    )


def inverse_temperature(logit):
    return 1.0 / (0.5 + jnp.maximum(logit, 0.0) + jnp.log(1.0 + jnp.exp(-jnp.abs(logit))))


def softmax_weights(logits):
    scaled = logits[0:G] * inverse_temperature(logits[G : G + 1] + logits[G + 1 : G + 2])
    e = jnp.exp(scaled - jnp.max(scaled, axis=0, keepdims=True))
    return (e * (1.0 / jnp.sum(e, axis=0, keepdims=True))).astype(BF16)


def kernel(
    x_hbm, entry_hbm, part_hbm, sharp_hbm, qkv_hbm, exit_hbm, wide_hbm, narrow_hbm,
    out_ref,
    xv, eh, part_ref, sharp_ref, qkv_ref, waug, pT, cs, f0, f1, acc, wall, nown, wT, wn, mbuf, yall, m0, m1, n0, n1,
    pair, plane, zbuf,
    x_sem, in_sem, own_sem, hop_sem, far_sem, d2d_sem, pair_sem, plane_sem, z_sem,
):
    pts, z = lax.axis_index("pts"), lax.axis_index("wid")
    core = lax.rem(pts, 2)
    gx, gy = pts // 8, lax.rem(pts // 2, 4)
    partner = pts + 1 - 2 * core

    def pts_at(dx, dy):
        return (lax.rem(gx + dx, 4) * 4 + lax.rem(gy + dy, 4)) * 2 + core

    def z_at(dz):
        return lax.rem(z + dz + H, H)

    def x_copy(i):
        return pltpu.make_async_copy(
            x_hbm.at[pl.ds(i * BLK, BLK)], xv.at[pl.ds(i * BLK, BLK)], x_sem.at[i]
        )

    entry_copy = pltpu.make_async_copy(entry_hbm, eh, in_sem.at[0])
    small_copies = [
        pltpu.make_async_copy(part_hbm, part_ref, in_sem.at[9]),
        pltpu.make_async_copy(sharp_hbm, sharp_ref, in_sem.at[10]),
    ]
    qkv_copy = pltpu.make_async_copy(qkv_hbm, qkv_ref, in_sem.at[11])
    entry_copy.start()
    for copy in small_copies:
        copy.start()
    x_copy(0).start()
    own_copies = []
    for k, ref in enumerate((entry_hbm, exit_hbm, wide_hbm, narrow_hbm)):
        for c in range(2):
            own_copies.append(
                pltpu.make_async_copy(
                    ref.at[pl.ds(c * HALF, HALF)], wall.at[k, z, c], in_sem.at[1 + 2 * k + c]
                )
            )

    for copy in own_copies:
        copy.start()
    qkv_copy.start()

    barrier = pltpu.get_barrier_semaphore()
    pl.semaphore_signal(barrier, inc=1, device_id=(partner, z), device_id_type=MESH)
    for dx, dy in PLANE[1:]:
        pl.semaphore_signal(barrier, inc=1, device_id=(pts_at(dx, dy), z), device_id_type=MESH)
    for dz in range(1, H):
        pl.semaphore_signal(barrier, inc=1, device_id=(pts, z_at(dz)), device_id_type=MESH)

    for copy in small_copies:
        copy.wait()
    sharp = jnp.broadcast_to(sharp_ref[...], (16, DH))
    sharp_hi = sharp.astype(BF16).astype(F32)
    row16 = lax.broadcasted_iota(jnp.int32, (16, DH), 0)
    tail = jnp.where(row16 == 0, sharp_hi, jnp.where(row16 == 1, sharp - sharp_hi, 0.0))
    table = jnp.concatenate([part_ref[...].astype(F32), tail], axis=0)
    blank = jnp.zeros((G + 16, DH), F32)
    pT[0 : G + 16, :] = jnp.concatenate([table, blank], axis=1).astype(BF16)
    pT[G + 16 :, :] = jnp.concatenate([blank, table], axis=1).astype(BF16)
    acc[...] = jnp.zeros_like(acc)

    for i in range(1, NBLK):
        x_copy(i).start()
    entry_copy.wait()
    head = eh[...].astype(F32)
    low = lax.broadcasted_iota(jnp.int32, (D, 128), 1) < DH
    both = jnp.concatenate([head, head], axis=0).T
    cs[...] = jnp.sum(both, axis=0, keepdims=True)
    for half, lanes in ((0, low), (1, jnp.logical_not(low))):
        waug[half * D : (half + 1) * D, 0:128] = jnp.where(lanes, both, 0.0).astype(BF16)
        waug[half * D : (half + 1) * D, 128:256] = jnp.where(lanes, 1.0 / D, 0.0).astype(BF16)

    def to(ref, sems, device, target=None):
        return pltpu.make_async_remote_copy(
            src_ref=ref, dst_ref=ref if target is None else target, send_sem=sems.at[0], recv_sem=sems.at[1],
            device_id=device, device_id_type=MESH,
        )

    def half_of(g, offset, half, rows=pl.ds(0, HALF)):
        return wall.at[g, z_at(offset), half, rows]

    def of_size(g, n, sems):
        return to(wall.at[g, pl.ds(0, n), 0], sems.at[g], (partner, z))

    def to_partner(g, offsets):
        for offset in offsets:
            to(half_of(g, offset, core), d2d_sem.at[g], (partner, z)).start()

    def weights_1():
        for copy in own_copies:
            copy.wait()
        for g in range(4):
            for d in (1, -1):
                to(half_of(g, 0, core), own_sem.at[g], (pts, z_at(d))).start()

    def weights_2(g):
        of_size(g, 2, own_sem).wait_recv()
        for d in (1, -1):
            to(half_of(g, -d, core), hop_sem.at[g], (pts, z_at(d))).start()

    def weights_3(g):
        of_size(g, 2, hop_sem).wait_recv()
        for d, first in ((1, 0), (-1, HALF // 2)):
            to(half_of(g, -2 * d, core), far_sem.at[g], (pts, z_at(d))).start()
            rows = pl.ds(first, HALF // 2)
            to(half_of(g, -2 * d, core, rows), far_sem.at[g], (pts, z_at(2 * d))).start()
        to_partner(g, (1, -1, 2, -2))

    def weights_far(g):
        of_size(g, 3, far_sem).wait_recv()
        to_partner(g, (3, -3, 4))

    def weights_done(g):
        of_size(g, 7, d2d_sem).wait_recv()

    def project(i, q, fbuf):
        start = i * BLK + q * DOT
        if not isinstance(start, int):
            start = pl.multiple_of(start, 32)
        first = xv[pl.ds(start, DOT), :]
        second = xv[pl.ds(start + PAIRS, DOT), :]
        y = jnp.dot(jnp.concatenate([first, second], axis=1), waug[...], preferred_element_type=F32)
        lower = lax.broadcasted_iota(jnp.int32, (16, 128), 1) < DH

        def square_sums(row):
            total = None
            for c in range(0, D, 128):
                tile = xv[pl.ds(row, 16), c : c + 128].astype(F32)
                total = tile * tile if total is None else total + tile * tile
            return jnp.broadcast_to(jnp.sum(total, axis=1, keepdims=True), (16, 128))

        for r in range(0, DOT, SUB):
            rows = slice(r, r + SUB)
            squares = []
            for k in range(r, r + SUB, 16):
                row = start + k if isinstance(start, int) else pl.multiple_of(start + k, 16)
                other = row + PAIRS if isinstance(start, int) else pl.multiple_of(row + PAIRS, 16)
                squares.append(jnp.where(lower, square_sums(row), square_sums(other)))
            squares = jnp.concatenate(squares, axis=0)
            mean = y[rows, 128:256]
            var = jnp.maximum(squares * (1.0 / D) - mean * mean, 0.0)
            feats = (y[rows, 0:128] - cs[...] * mean) * lax.rsqrt(var + 1e-05)
            fbuf[q * DOT + r : q * DOT + r + SUB, :] = feats.astype(BF16)
            yield

    def slices(fbuf):
        logits = contract_lanes(pT[...], fbuf[...])
        yield
        exps = []
        for top in (0, G + 16):
            scaled = logits[top : top + G] * inverse_temperature(
                logits[top + G : top + G + 1] + logits[top + G + 1 : top + G + 2]
            )
            exps.append(jnp.exp(scaled - jnp.max(scaled, axis=0, keepdims=True)))
        yield
        w = [(e * (1.0 / jnp.sum(e, axis=0, keepdims=True))).astype(BF16) for e in exps]
        yield
        with_ones = jnp.concatenate([fbuf[...], jnp.ones((PAIRS, 128), BF16)], axis=1)
        acc[...] += jnp.dot(jnp.concatenate(w, axis=0), with_ones, preferred_element_type=F32)
        yield

    def project_and_slices(i, fbuf, other):
        steps = slices(other)
        for q in range(PAIRS // DOT):
            for _ in project(i, q, fbuf):
                next(steps)

    x_copy(0).wait()
    for q in range(PAIRS // DOT):
        for _ in project(0, q, f0):
            pass

    start_at = (z < 1).astype(jnp.int32) + (z < 4).astype(jnp.int32)

    def two_blocks(j, _):
        @pl.when(j == start_at)
        def _():
            pl.semaphore_wait(barrier, 1 + 15 + 7)
            weights_1()

        x_copy(2 * j + 1).wait()
        x_copy(2 * j + 2).wait()
        project_and_slices(2 * j + 1, f1, f0)
        project_and_slices(2 * j + 2, f0, f1)
        return 0

    lax.fori_loop(0, NBLK // 2 - 1, two_blocks, 0)
    weights_2(0)
    weights_2(1)
    x_copy(NBLK - 1).wait()
    project_and_slices(NBLK - 1, f1, f0)
    weights_2(2)
    weights_2(3)
    for _ in slices(f1):
        pass

    half_g = G // 2
    lane = lax.broadcasted_iota(jnp.int32, (G, 128), 1)
    diagonal = lane == lax.broadcasted_iota(jnp.int32, (G, 128), 0)
    even, odd = acc[0:G, 0:128], acc[G:, 0:128]
    straight, crossed = even + pltpu.roll(odd, DH, axis=1), pltpu.roll(even, DH, axis=1) + odd
    mass = acc[0:G, 128:256] + acc[G:, 128:256]
    pair[0, 0:half_g, :] = jnp.where(lane[0:half_g] < DH, straight[0:half_g], crossed[half_g:])
    pair[0, half_g : half_g + 1, :] = jnp.sum(jnp.where(diagonal, mass, 0.0), axis=0, keepdims=True)
    pair_copy = to(pair.at[0], pair_sem, (partner, z), pair.at[1])
    pair_copy.start()
    pair_copy.wait_recv()
    plane[0] = pair[0] + pair[1]
    for r in range(1, 16):
        to(plane.at[0], plane_sem, (pts_at(*PLANE[r]), z), plane.at[r]).start()
    plane_all = to(plane.at[pl.ds(1, 15)], plane_sem, (partner, z))

    weights_3(0)
    own = pl.multiple_of(z * OWN, 128)

    def own_norm(t, _):
        rows = xv[pl.ds(pl.multiple_of(own + t * NORM_ROWS, 32), NORM_ROWS), :].astype(F32)
        centred = rows - jnp.mean(rows, axis=1, keepdims=True)
        var = jnp.mean(centred * centred, axis=1, keepdims=True)
        nown[pl.ds(pl.multiple_of(t * NORM_ROWS, 32), NORM_ROWS), :] = (centred * lax.rsqrt(var + 1e-05)).astype(BF16)
        return 0

    lax.fori_loop(0, OWN // NORM_ROWS, own_norm, 0)
    for g in range(1, 4):
        weights_3(g)
    weights_far(0)

    qkv_copy.wait()
    plane_all.wait_recv()
    sums = jnp.sum(plane[...], axis=0)
    packed = sums[0:half_g]
    numerator = jnp.concatenate([packed, pltpu.roll(packed, DH, axis=1)], axis=0)[:, 0:DH]
    mass = jnp.sum(jnp.where(diagonal, sums[half_g : half_g + 1], 0.0), axis=1, keepdims=True)
    tokens = numerator / (mass + 1e-05)
    maps = jnp.concatenate([qkv_ref[0], qkv_ref[1], qkv_ref[2], qkv_ref[2]], axis=1)
    mapped = jnp.dot(tokens, maps, preferred_element_type=F32, precision=HIGH)
    scores = contract_lanes(mapped[:, 0:DH], mapped[:, DH : 2 * DH], precision=HIGH) * 0.125
    values = jnp.where((lane < DH) == (lax.rem(z, 2) == 0), mapped[:, 2 * DH : 4 * DH], 0.0)
    e = jnp.exp(scores - jnp.max(scores, axis=1, keepdims=True))
    attend = e / jnp.sum(e, axis=1, keepdims=True)
    zbuf[z] = jnp.dot(attend, values, preferred_element_type=F32, precision=HIGH).astype(BF16)

    for dz in range(1, H):
        to(zbuf.at[z], z_sem, (pts, z_at(dz))).start()
    z_all = to(zbuf.at[pl.ds(0, H - 1)], z_sem, (partner, z))

    weights_far(1)
    weights_done(0)
    yall[...] = contract_lanes(wall[0].reshape(D, D), nown[...]).astype(BF16)
    for h in range(H):
        if h == 2:
            weights_far(2)
        if h == 5:
            weights_far(3)
        logits = jnp.dot(pT[0 : G + 16, 0:DH], yall[h * DH : (h + 1) * DH, :], preferred_element_type=F32)
        wT[h * G : (h + 1) * G, :] = softmax_weights(logits)
    wn[...] = wT[...].T
    z_all.wait_recv()
    weights_done(1)

    gap = jnp.zeros((2 * G, 128), BF16)
    for h in range(0, H, 4):
        first, second = (zbuf[k : k + 2].reshape(2 * G, 128) for k in (h, h + 2))
        tokens_of_four = jnp.concatenate(
            [jnp.concatenate([first, gap], axis=1), jnp.concatenate([gap, second], axis=1)], axis=0
        )
        mbuf[h * G : (h + 4) * G, :] = jnp.dot(
            tokens_of_four, wall[1, h : h + 4].reshape(4 * DH, D), preferred_element_type=F32
        ).astype(BF16)

    def mix(t, mid, normed):
        x_rows = xv[pl.ds(pl.multiple_of(own + t * TBLK, 32), TBLK), :].astype(F32)
        midway = x_rows + jnp.dot(wn[t * TBLK : (t + 1) * TBLK, :], mbuf[...], preferred_element_type=F32)
        centred = midway - jnp.mean(midway, axis=1, keepdims=True)
        var = jnp.mean(centred * centred, axis=1, keepdims=True)
        mid[...] = midway
        normed[...] = (centred * lax.rsqrt(var + 1e-05)).astype(BF16)

    def feed(t, mid, normed):
        hidden = jnp.dot(normed[...], wall[2].reshape(D, D), preferred_element_type=F32)
        hidden = jax.nn.gelu(hidden).astype(BF16)
        out = mid[...] + jnp.dot(hidden, wall[3].reshape(D, D), preferred_element_type=F32)
        out_ref[t * TBLK : (t + 1) * TBLK, :] = out.astype(BF16)

    stage = ((m0, n0), (m1, n1))
    mix(0, *stage[0])
    weights_done(2)
    weights_done(3)
    for t in range(OWN // TBLK):
        if t + 1 < OWN // TBLK:
            mix(t + 1, *stage[(t + 1) % 2])
        feed(t, *stage[t % 2])

    for g in range(4):
        of_size(g, 2, own_sem).wait_send()
        of_size(g, 2, hop_sem).wait_send()
        of_size(g, 3, far_sem).wait_send()
        of_size(g, 7, d2d_sem).wait_send()
    pair_copy.wait_send()
    plane_all.wait_send()
    z_all.wait_send()


OUT = pltpu.VMEM((OWN, D), BF16)


def local(x, entry, partition, sharpness, qkv, exit_matrix, widening, narrowing):
    hbm = pl.BlockSpec(memory_space=pl.ANY)
    vmem = pl.BlockSpec(memory_space=pltpu.VMEM)
    dma = pltpu.SemaphoreType.DMA
    return pl.pallas_call(
        kernel,
        out_shape=OUT,
        in_specs=[hbm] * 8,
        out_specs=vmem,
        scratch_shapes=[
            pltpu.VMEM((ROWS, D), BF16),
            pltpu.VMEM((DH, D), BF16),
            pltpu.VMEM((G, DH), BF16),
            pltpu.VMEM((1, DH), F32),
            pltpu.VMEM((3, DH, DH), F32),
            pltpu.VMEM((2 * D, 256), BF16),
            pltpu.VMEM((2 * (G + 16), 128), BF16),
            pltpu.VMEM((1, 128), F32),
            pltpu.VMEM((PAIRS, 128), BF16),
            pltpu.VMEM((PAIRS, 128), BF16),
            pltpu.VMEM((2 * G, 256), F32),
            pltpu.VMEM((4, H, 2, HALF, D), BF16),
            pltpu.VMEM((OWN, D), BF16),
            pltpu.VMEM((H * G, OWN), BF16),
            pltpu.VMEM((OWN, H * G), BF16),
            pltpu.VMEM((H * G, D), BF16),
            pltpu.VMEM((D, OWN), BF16),
            pltpu.VMEM((TBLK, D), F32),
            pltpu.VMEM((TBLK, D), F32),
            pltpu.VMEM((TBLK, D), BF16),
            pltpu.VMEM((TBLK, D), BF16),
            pltpu.VMEM((2, G // 2 + 1, 128), F32),
            pltpu.VMEM((16, G // 2 + 1, 128), F32),
            pltpu.VMEM((H, G, 128), BF16),
            dma((NBLK,)),
            dma((12,)),
            dma((4, 2)),
            dma((4, 2)),
            dma((4, 2)),
            dma((4, 2)),
            dma((2,)),
            dma((2,)),
            dma((2,)),
        ],
        compiler_params=pltpu.CompilerParams(
            collective_id=0, has_side_effects=True, vmem_limit_bytes=60 * 2**20
        ),
    )(x, entry.T, partition.T, sharpness.reshape(1, DH), qkv, exit_matrix, widening, narrowing)


def solution(mesh):
    placed = (
        P("pts", None), P(None, "wid"), P(), P(), P(),
        P("wid", None), P("wid", None), P("wid", None),
    )
    return jax.shard_map(
        local, mesh=mesh, in_specs=placed, out_specs=P(("pts", "wid"), None), check_vma=False
    )
```

```python
import functools

import jax
import jax.numpy as jnp
from jax import lax
from jax.experimental import pallas as pl
from jax.experimental.pallas import tpu as pltpu
from jax.sharding import PartitionSpec as P

MESH = pl.DeviceIdType.MESH
F32, BF16 = jnp.float32, jnp.bfloat16
HIGH = lax.Precision.HIGHEST

D, H, DH, G = 512, 8, 64, 32
ROWS = 11264
OWN = 1408
BLK = 1408
PAIRS = BLK // 2
DOT = 352
SUB = 176
NBLK = ROWS // BLK
NORM_ROWS = 352
TBLK = 704
HALF = DH // 2

PLANE = [(dx, dy) for dx in range(4) for dy in range(4)]


def contract_lanes(a, b, precision=None):
    return lax.dot_general(
        a, b, (((1,), (1,)), ((), ())), preferred_element_type=F32, precision=precision
    )


def inverse_temperature(logit):
    return 1.0 / (0.5 + jnp.maximum(logit, 0.0) + jnp.log(1.0 + jnp.exp(-jnp.abs(logit))))


def softmax_weights(logits):
    scaled = logits[0:G] * inverse_temperature(logits[G : G + 1] + logits[G + 1 : G + 2])
    e = jnp.exp(scaled - jnp.max(scaled, axis=0, keepdims=True))
    return (e * (1.0 / jnp.sum(e, axis=0, keepdims=True))).astype(BF16)


def kernel(
    x_hbm, entry_hbm, part_hbm, sharp_hbm, qkv_hbm, exit_hbm, wide_hbm, narrow_hbm,
    out_ref,
    xv, eh, part_ref, sharp_ref, qkv_ref, waug, pT, cs, f0, f1, acc, wall, nown, wT, wn, mbuf, yall, m0, m1, n0, n1,
    pair, plane, zbuf,
    x_sem, in_sem, own_sem, hop_sem, far_sem, d2d_sem, pair_sem, plane_sem, z_sem,
):
    pts, z = lax.axis_index("pts"), lax.axis_index("wid")
    core = lax.rem(pts, 2)
    gx, gy = pts // 8, lax.rem(pts // 2, 4)
    partner = pts + 1 - 2 * core

    def pts_at(dx, dy):
        return (lax.rem(gx + dx, 4) * 4 + lax.rem(gy + dy, 4)) * 2 + core

    def z_at(dz):
        return lax.rem(z + dz + H, H)

    def x_copy(i):
        return pltpu.make_async_copy(
            x_hbm.at[pl.ds(i * BLK, BLK)], xv.at[pl.ds(i * BLK, BLK)], x_sem.at[i]
        )

    entry_copy = pltpu.make_async_copy(entry_hbm, eh, in_sem.at[0])
    small_copies = [
        pltpu.make_async_copy(part_hbm, part_ref, in_sem.at[9]),
        pltpu.make_async_copy(sharp_hbm, sharp_ref, in_sem.at[10]),
    ]
    qkv_copy = pltpu.make_async_copy(qkv_hbm, qkv_ref, in_sem.at[11])
    entry_copy.start()
    for copy in small_copies:
        copy.start()
    x_copy(0).start()
    own_copies = []
    for k, ref in enumerate((entry_hbm, exit_hbm, wide_hbm, narrow_hbm)):
        for c in range(2):
            own_copies.append(
                pltpu.make_async_copy(
                    ref.at[pl.ds(c * HALF, HALF)], wall.at[k, z, c], in_sem.at[1 + 2 * k + c]
                )
            )

    for copy in own_copies:
        copy.start()
    qkv_copy.start()

    barrier = pltpu.get_barrier_semaphore()
    pl.semaphore_signal(barrier, inc=1, device_id=(partner, z), device_id_type=MESH)
    for dx, dy in PLANE[1:]:
        pl.semaphore_signal(barrier, inc=1, device_id=(pts_at(dx, dy), z), device_id_type=MESH)
    for dz in range(1, H):
        pl.semaphore_signal(barrier, inc=1, device_id=(pts, z_at(dz)), device_id_type=MESH)

    for copy in small_copies:
        copy.wait()
    sharp = jnp.broadcast_to(sharp_ref[...], (16, DH))
    sharp_hi = sharp.astype(BF16).astype(F32)
    row16 = lax.broadcasted_iota(jnp.int32, (16, DH), 0)
    tail = jnp.where(row16 == 0, sharp_hi, jnp.where(row16 == 1, sharp - sharp_hi, 0.0))
    table = jnp.concatenate([part_ref[...].astype(F32), tail], axis=0)
    blank = jnp.zeros((G + 16, DH), F32)
    pT[0 : G + 16, :] = jnp.concatenate([table, blank], axis=1).astype(BF16)
    pT[G + 16 :, :] = jnp.concatenate([blank, table], axis=1).astype(BF16)
    acc[...] = jnp.zeros_like(acc)

    for i in range(1, NBLK):
        x_copy(i).start()
    entry_copy.wait()
    head = eh[...].astype(F32)
    low = lax.broadcasted_iota(jnp.int32, (D, 128), 1) < DH
    both = jnp.concatenate([head, head], axis=0).T
    cs[...] = jnp.sum(both, axis=0, keepdims=True)
    for half, lanes in ((0, low), (1, jnp.logical_not(low))):
        waug[half * D : (half + 1) * D, 0:128] = jnp.where(lanes, both, 0.0).astype(BF16)
        waug[half * D : (half + 1) * D, 128:256] = jnp.where(lanes, 1.0 / D, 0.0).astype(BF16)

    def to(ref, sems, device, target=None):
        return pltpu.make_async_remote_copy(
            src_ref=ref, dst_ref=ref if target is None else target, send_sem=sems.at[0], recv_sem=sems.at[1],
            device_id=device, device_id_type=MESH,
        )

    def half_of(g, offset, half, rows=pl.ds(0, HALF)):
        return wall.at[g, z_at(offset), half, rows]

    def of_size(g, n, sems):
        return to(wall.at[g, pl.ds(0, n), 0], sems.at[g], (partner, z))

    def to_partner(g, offsets):
        for offset in offsets:
            to(half_of(g, offset, core), d2d_sem.at[g], (partner, z)).start()

    def weights_1():
        for copy in own_copies:
            copy.wait()
        for g in range(4):
            for d in (1, -1):
                to(half_of(g, 0, core), own_sem.at[g], (pts, z_at(d))).start()

    def weights_2(g):
        of_size(g, 2, own_sem).wait_recv()
        for d in (1, -1):
            to(half_of(g, -d, core), hop_sem.at[g], (pts, z_at(d))).start()

    def weights_3(g):
        of_size(g, 2, hop_sem).wait_recv()
        for d, first in ((1, 0), (-1, HALF // 2)):
            to(half_of(g, -2 * d, core), far_sem.at[g], (pts, z_at(d))).start()
            rows = pl.ds(first, HALF // 2)
            to(half_of(g, -2 * d, core, rows), far_sem.at[g], (pts, z_at(2 * d))).start()
        to_partner(g, (1, -1, 2, -2))

    def weights_far(g):
        of_size(g, 3, far_sem).wait_recv()
        to_partner(g, (3, -3, 4))

    def weights_done(g):
        of_size(g, 7, d2d_sem).wait_recv()

    def project(i, q, fbuf):
        start = i * BLK + q * DOT
        if not isinstance(start, int):
            start = pl.multiple_of(start, 32)
        first = xv[pl.ds(start, DOT), :]
        second = xv[pl.ds(start + PAIRS, DOT), :]
        y = jnp.dot(jnp.concatenate([first, second], axis=1), waug[...], preferred_element_type=F32)
        lower = lax.broadcasted_iota(jnp.int32, (16, 128), 1) < DH

        def square_sums(row):
            total = None
            for c in range(0, D, 128):
                tile = xv[pl.ds(row, 16), c : c + 128].astype(F32)
                total = tile * tile if total is None else total + tile * tile
            return jnp.broadcast_to(jnp.sum(total, axis=1, keepdims=True), (16, 128))

        for r in range(0, DOT, SUB):
            rows = slice(r, r + SUB)
            squares = []
            for k in range(r, r + SUB, 16):
                row = start + k if isinstance(start, int) else pl.multiple_of(start + k, 16)
                other = row + PAIRS if isinstance(start, int) else pl.multiple_of(row + PAIRS, 16)
                squares.append(jnp.where(lower, square_sums(row), square_sums(other)))
            squares = jnp.concatenate(squares, axis=0)
            mean = y[rows, 128:256]
            var = jnp.maximum(squares * (1.0 / D) - mean * mean, 0.0)
            feats = (y[rows, 0:128] - cs[...] * mean) * lax.rsqrt(var + 1e-05)
            fbuf[q * DOT + r : q * DOT + r + SUB, :] = feats.astype(BF16)
            yield

    def slices(fbuf):
        logits = contract_lanes(pT[...], fbuf[...])
        yield
        exps = []
        for top in (0, G + 16):
            scaled = logits[top : top + G] * inverse_temperature(
                logits[top + G : top + G + 1] + logits[top + G + 1 : top + G + 2]
            )
            exps.append(jnp.exp(scaled - jnp.max(scaled, axis=0, keepdims=True)))
        yield
        w = [(e * (1.0 / jnp.sum(e, axis=0, keepdims=True))).astype(BF16) for e in exps]
        yield
        with_ones = jnp.concatenate([fbuf[...], jnp.ones((PAIRS, 128), BF16)], axis=1)
        acc[...] += jnp.dot(jnp.concatenate(w, axis=0), with_ones, preferred_element_type=F32)
        yield

    def project_and_slices(i, fbuf, other):
        steps = slices(other)
        for q in range(PAIRS // DOT):
            for _ in project(i, q, fbuf):
                next(steps)

    x_copy(0).wait()
    for q in range(PAIRS // DOT):
        for _ in project(0, q, f0):
            pass

    start_at = (z < 1).astype(jnp.int32) + (z < 4).astype(jnp.int32)

    def two_blocks(j, _):
        @pl.when(j == start_at)
        def _():
            pl.semaphore_wait(barrier, 1 + 15 + 7)
            weights_1()

        x_copy(2 * j + 1).wait()
        x_copy(2 * j + 2).wait()
        project_and_slices(2 * j + 1, f1, f0)
        project_and_slices(2 * j + 2, f0, f1)
        return 0

    lax.fori_loop(0, NBLK // 2 - 1, two_blocks, 0)
    weights_2(0)
    weights_2(1)
    x_copy(NBLK - 1).wait()
    project_and_slices(NBLK - 1, f1, f0)
    weights_2(2)
    weights_2(3)
    for _ in slices(f1):
        pass

    half_g = G // 2
    lane = lax.broadcasted_iota(jnp.int32, (G, 128), 1)
    diagonal = lane == lax.broadcasted_iota(jnp.int32, (G, 128), 0)
    even, odd = acc[0:G, 0:128], acc[G:, 0:128]
    straight, crossed = even + pltpu.roll(odd, DH, axis=1), pltpu.roll(even, DH, axis=1) + odd
    mass = acc[0:G, 128:256] + acc[G:, 128:256]
    pair[0, 0:half_g, :] = jnp.where(lane[0:half_g] < DH, straight[0:half_g], crossed[half_g:])
    pair[0, half_g : half_g + 1, :] = jnp.sum(jnp.where(diagonal, mass, 0.0), axis=0, keepdims=True)
    pair_copy = to(pair.at[0], pair_sem, (partner, z), pair.at[1])
    plane_all = to(plane.at[pl.ds(1, 15)], plane_sem, (partner, z))

    @pl.when(core == 0)
    def _():
        pair_copy.start()

    @pl.when(core == 1)
    def _():
        pair_copy.wait_recv()
        plane[0] = pair[0] + pair[1]
        for r in range(1, 16):
            to(plane.at[0], plane_sem, (pts_at(*PLANE[r]), z), plane.at[r]).start()

    weights_3(0)
    own = pl.multiple_of(z * OWN, 128)

    def own_norm(t, _):
        rows = xv[pl.ds(pl.multiple_of(own + t * NORM_ROWS, 32), NORM_ROWS), :].astype(F32)
        centred = rows - jnp.mean(rows, axis=1, keepdims=True)
        var = jnp.mean(centred * centred, axis=1, keepdims=True)
        nown[pl.ds(pl.multiple_of(t * NORM_ROWS, 32), NORM_ROWS), :] = (centred * lax.rsqrt(var + 1e-05)).astype(BF16)
        return 0

    lax.fori_loop(0, OWN // NORM_ROWS, own_norm, 0)
    for g in range(1, 4):
        weights_3(g)
    weights_far(0)

    qkv_copy.wait()

    @pl.when(core == 1)
    def _():
        plane_all.wait_recv()
        sums = jnp.sum(plane[...], axis=0)
        packed = sums[0:half_g]
        numerator = jnp.concatenate([packed, pltpu.roll(packed, DH, axis=1)], axis=0)[:, 0:DH]
        mass = jnp.sum(jnp.where(diagonal, sums[half_g : half_g + 1], 0.0), axis=1, keepdims=True)
        tokens = numerator / (mass + 1e-05)
        maps = jnp.concatenate([qkv_ref[0], qkv_ref[1], qkv_ref[2], qkv_ref[2]], axis=1)
        mapped = jnp.dot(tokens, maps, preferred_element_type=F32, precision=HIGH)
        scores = contract_lanes(mapped[:, 0:DH], mapped[:, DH : 2 * DH], precision=HIGH) * 0.125
        values = jnp.where((lane < DH) == (lax.rem(z, 2) == 0), mapped[:, 2 * DH : 4 * DH], 0.0)
        e = jnp.exp(scores - jnp.max(scores, axis=1, keepdims=True))
        attend = e / jnp.sum(e, axis=1, keepdims=True)
        zbuf[z] = jnp.dot(attend, values, preferred_element_type=F32, precision=HIGH).astype(BF16)

        for dz in range(1, H):
            to(zbuf.at[z], z_sem, (pts, z_at(dz))).start()

    def z_of(n):
        return to(zbuf.at[pl.ds(0, n)], z_sem, (partner, z))

    weights_done(0)
    yall[...] = contract_lanes(wall[0].reshape(D, D), nown[...]).astype(BF16)
    weights_far(1)
    for h in range(H):
        if h == 2:
            weights_far(2)
        if h == 5:
            weights_far(3)
        logits = jnp.dot(pT[0 : G + 16, 0:DH], yall[h * DH : (h + 1) * DH, :], preferred_element_type=F32)
        wT[h * G : (h + 1) * G, :] = softmax_weights(logits)
    wn[...] = wT[...].T
    @pl.when(core == 1)
    def _():
        z_of(H - 1).wait_recv()
        to(zbuf, z_sem, (partner, z)).start()

    @pl.when(core == 0)
    def _():
        z_of(H).wait_recv()

    weights_done(1)

    gap = jnp.zeros((2 * G, 128), BF16)
    for h in range(0, H, 4):
        first, second = (zbuf[k : k + 2].reshape(2 * G, 128) for k in (h, h + 2))
        tokens_of_four = jnp.concatenate(
            [jnp.concatenate([first, gap], axis=1), jnp.concatenate([gap, second], axis=1)], axis=0
        )
        mbuf[h * G : (h + 4) * G, :] = jnp.dot(
            tokens_of_four, wall[1, h : h + 4].reshape(4 * DH, D), preferred_element_type=F32
        ).astype(BF16)

    def mix(t, mid, normed):
        x_rows = xv[pl.ds(pl.multiple_of(own + t * TBLK, 32), TBLK), :].astype(F32)
        midway = x_rows + jnp.dot(wn[t * TBLK : (t + 1) * TBLK, :], mbuf[...], preferred_element_type=F32)
        centred = midway - jnp.mean(midway, axis=1, keepdims=True)
        var = jnp.mean(centred * centred, axis=1, keepdims=True)
        mid[...] = midway
        normed[...] = (centred * lax.rsqrt(var + 1e-05)).astype(BF16)

    def feed(t, mid, normed):
        hidden = jnp.dot(normed[...], wall[2].reshape(D, D), preferred_element_type=F32)
        hidden = jax.nn.gelu(hidden).astype(BF16)
        out = mid[...] + jnp.dot(hidden, wall[3].reshape(D, D), preferred_element_type=F32)
        out_ref[t * TBLK : (t + 1) * TBLK, :] = out.astype(BF16)

    stage = ((m0, n0), (m1, n1))
    mix(0, *stage[0])
    weights_done(2)
    weights_done(3)
    for t in range(OWN // TBLK):
        if t + 1 < OWN // TBLK:
            mix(t + 1, *stage[(t + 1) % 2])
        feed(t, *stage[t % 2])

    for g in range(4):
        of_size(g, 2, own_sem).wait_send()
        of_size(g, 2, hop_sem).wait_send()
        of_size(g, 3, far_sem).wait_send()
        of_size(g, 7, d2d_sem).wait_send()

    @pl.when(core == 0)
    def _():
        pair_copy.wait_send()

    @pl.when(core == 1)
    def _():
        plane_all.wait_send()
        z_of(H).wait_send()
        z_of(H - 1).wait_send()


OUT = pltpu.VMEM((OWN, D), BF16)


def local(x, entry, partition, sharpness, qkv, exit_matrix, widening, narrowing):
    hbm = pl.BlockSpec(memory_space=pl.ANY)
    vmem = pl.BlockSpec(memory_space=pltpu.VMEM)
    dma = pltpu.SemaphoreType.DMA
    return pl.pallas_call(
        kernel,
        out_shape=OUT,
        in_specs=[hbm] * 8,
        out_specs=vmem,
        scratch_shapes=[
            pltpu.VMEM((ROWS, D), BF16),
            pltpu.VMEM((DH, D), BF16),
            pltpu.VMEM((G, DH), BF16),
            pltpu.VMEM((1, DH), F32),
            pltpu.VMEM((3, DH, DH), F32),
            pltpu.VMEM((2 * D, 256), BF16),
            pltpu.VMEM((2 * (G + 16), 128), BF16),
            pltpu.VMEM((1, 128), F32),
            pltpu.VMEM((PAIRS, 128), BF16),
            pltpu.VMEM((PAIRS, 128), BF16),
            pltpu.VMEM((2 * G, 256), F32),
            pltpu.VMEM((4, H, 2, HALF, D), BF16),
            pltpu.VMEM((OWN, D), BF16),
            pltpu.VMEM((H * G, OWN), BF16),
            pltpu.VMEM((OWN, H * G), BF16),
            pltpu.VMEM((H * G, D), BF16),
            pltpu.VMEM((D, OWN), BF16),
            pltpu.VMEM((TBLK, D), F32),
            pltpu.VMEM((TBLK, D), F32),
            pltpu.VMEM((TBLK, D), BF16),
            pltpu.VMEM((TBLK, D), BF16),
            pltpu.VMEM((2, G // 2 + 1, 128), F32),
            pltpu.VMEM((16, G // 2 + 1, 128), F32),
            pltpu.VMEM((H, G, 128), BF16),
            dma((NBLK,)),
            dma((12,)),
            dma((4, 2)),
            dma((4, 2)),
            dma((4, 2)),
            dma((4, 2)),
            dma((2,)),
            dma((2,)),
            dma((2,)),
        ],
        compiler_params=pltpu.CompilerParams(
            collective_id=0, has_side_effects=True, vmem_limit_bytes=60 * 2**20
        ),
    )(x, entry.T, partition.T, sharpness.reshape(1, DH), qkv, exit_matrix, widening, narrowing)


def solution(mesh):
    placed = (
        P("pts", None), P(None, "wid"), P(), P(), P(),
        P("wid", None), P("wid", None), P("wid", None),
    )
    return jax.shard_map(
        local, mesh=mesh, in_specs=placed, out_specs=P(("pts", "wid"), None), check_vma=False
    )
```

```python
import functools

import jax
import jax.numpy as jnp
from jax import lax
from jax.experimental import pallas as pl
from jax.experimental.pallas import tpu as pltpu
from jax.sharding import PartitionSpec as P

MESH = pl.DeviceIdType.MESH
F32, BF16 = jnp.float32, jnp.bfloat16
HIGH = lax.Precision.HIGHEST

D, H, DH, G = 512, 8, 64, 32
ROWS = 11264
OWN = 1408
BLK = 1408
PAIRS = BLK // 2
DOT = 352
SUB = 176
NBLK = ROWS // BLK
NORM_ROWS = 352
TBLK = 704
HALF = DH // 2

PLANE = [(dx, dy) for dx in range(4) for dy in range(4)]


def contract_lanes(a, b, precision=None):
    return lax.dot_general(
        a, b, (((1,), (1,)), ((), ())), preferred_element_type=F32, precision=precision
    )


def inverse_temperature(logit):
    return 1.0 / (0.5 + jnp.maximum(logit, 0.0) + jnp.log(1.0 + jnp.exp(-jnp.abs(logit))))


def softmax_weights(logits):
    scaled = logits[0:G] * inverse_temperature(logits[G : G + 1] + logits[G + 1 : G + 2])
    e = jnp.exp(scaled - jnp.max(scaled, axis=0, keepdims=True))
    return (e * (1.0 / jnp.sum(e, axis=0, keepdims=True))).astype(BF16)


def kernel(
    x_hbm, entry_hbm, part_hbm, sharp_hbm, qkv_hbm, exit_hbm, wide_hbm, narrow_hbm,
    out_ref,
    xv, eh, part_ref, sharp_ref, qkv_ref, waug, pT, cs, f0, f1, acc, wall, nown, wT, wn, mbuf, yall, m0, m1, n0, n1,
    pair, plane, zbuf,
    x_sem, in_sem, own_sem, hop_sem, far_sem, d2d_sem, pair_sem, plane_sem, z_sem,
):
    pts, z = lax.axis_index("pts"), lax.axis_index("wid")
    core = lax.rem(pts, 2)
    gx, gy = pts // 8, lax.rem(pts // 2, 4)
    partner = pts + 1 - 2 * core

    def pts_at(dx, dy):
        return (lax.rem(gx + dx, 4) * 4 + lax.rem(gy + dy, 4)) * 2 + core

    def z_at(dz):
        return lax.rem(z + dz + H, H)

    def x_copy(i):
        return pltpu.make_async_copy(
            x_hbm.at[pl.ds(i * BLK, BLK)], xv.at[pl.ds(i * BLK, BLK)], x_sem.at[i]
        )

    entry_copy = pltpu.make_async_copy(entry_hbm, eh, in_sem.at[0])
    small_copies = [
        pltpu.make_async_copy(part_hbm, part_ref, in_sem.at[9]),
        pltpu.make_async_copy(sharp_hbm, sharp_ref, in_sem.at[10]),
    ]
    qkv_copy = pltpu.make_async_copy(qkv_hbm, qkv_ref, in_sem.at[11])
    entry_copy.start()
    for copy in small_copies:
        copy.start()
    x_copy(0).start()
    own_copies = []
    for k, ref in enumerate((entry_hbm, exit_hbm, wide_hbm, narrow_hbm)):
        for c in range(2):
            own_copies.append(
                pltpu.make_async_copy(
                    ref.at[pl.ds(c * HALF, HALF)], wall.at[k, z, c], in_sem.at[1 + 2 * k + c]
                )
            )

    for copy in own_copies:
        copy.start()
    qkv_copy.start()

    barrier = pltpu.get_barrier_semaphore()
    pl.semaphore_signal(barrier, inc=1, device_id=(partner, z), device_id_type=MESH)
    for dx, dy in PLANE[1:]:
        pl.semaphore_signal(barrier, inc=1, device_id=(pts_at(dx, dy), z), device_id_type=MESH)
    for dz in range(1, H):
        pl.semaphore_signal(barrier, inc=1, device_id=(pts, z_at(dz)), device_id_type=MESH)

    for copy in small_copies:
        copy.wait()
    sharp = jnp.broadcast_to(sharp_ref[...], (16, DH))
    sharp_hi = sharp.astype(BF16).astype(F32)
    row16 = lax.broadcasted_iota(jnp.int32, (16, DH), 0)
    tail = jnp.where(row16 == 0, sharp_hi, jnp.where(row16 == 1, sharp - sharp_hi, 0.0))
    table = jnp.concatenate([part_ref[...].astype(F32), tail], axis=0)
    blank = jnp.zeros((G + 16, DH), F32)
    pT[0 : G + 16, :] = jnp.concatenate([table, blank], axis=1).astype(BF16)
    pT[G + 16 :, :] = jnp.concatenate([blank, table], axis=1).astype(BF16)
    acc[...] = jnp.zeros_like(acc)

    for i in range(1, NBLK):
        x_copy(i).start()
    entry_copy.wait()
    head = eh[...].astype(F32)
    low = lax.broadcasted_iota(jnp.int32, (D, 128), 1) < DH
    both = jnp.concatenate([head, head], axis=0).T
    cs[...] = jnp.sum(both, axis=0, keepdims=True)
    for half, lanes in ((0, low), (1, jnp.logical_not(low))):
        waug[half * D : (half + 1) * D, 0:128] = jnp.where(lanes, both, 0.0).astype(BF16)
        waug[half * D : (half + 1) * D, 128:256] = jnp.where(lanes, 1.0 / D, 0.0).astype(BF16)

    carrier = {0: 1, 1: 0, 2: 1, 3: 0}

    def to(ref, sems, device, target=None):
        return pltpu.make_async_remote_copy(
            src_ref=ref, dst_ref=ref if target is None else target, send_sem=sems.at[0], recv_sem=sems.at[1],
            device_id=device, device_id_type=MESH,
        )

    def by_carrier(g, act, other=False):
        if g in carrier:
            pl.when(core == (1 - carrier[g] if other else carrier[g]))(act)
        else:
            act()

    def piece(g, offset, side=None):
        shard = z_at(offset)
        if g in carrier:
            return wall.at[g, shard] if side is None else wall.at[g, shard, side]
        rows = pl.ds(0, HALF) if side is None else pl.ds(side * (HALF // 2), HALF // 2)
        return wall.at[g, shard, core, rows]

    def of_size(g, n, sems):
        some = wall.at[g, pl.ds(0, n)] if g in carrier else wall.at[g, pl.ds(0, n), 0]
        return to(some, sems.at[g], (partner, z))

    def to_partner(g, offsets):
        for offset in offsets:
            to(piece(g, offset), d2d_sem.at[g], (partner, z)).start()

    def weights_1():
        for copy in own_copies:
            copy.wait()
        for g in range(4):

            def act(g=g):
                for d in (1, -1):
                    to(piece(g, 0), own_sem.at[g], (pts, z_at(d))).start()

            by_carrier(g, act)

    def weights_2(g):
        def act():
            of_size(g, 2, own_sem).wait_recv()
            for d in (1, -1):
                to(piece(g, -d), hop_sem.at[g], (pts, z_at(d))).start()

        by_carrier(g, act)

    def weights_3(g):
        def act():
            of_size(g, 2, hop_sem).wait_recv()
            for d, side in ((1, 0), (-1, 1)):
                to(piece(g, -2 * d), far_sem.at[g], (pts, z_at(d))).start()
                to(piece(g, -2 * d, side), far_sem.at[g], (pts, z_at(2 * d))).start()
            to_partner(g, (1, -1, 2, -2))

        by_carrier(g, act)

    def weights_far(g):
        def act():
            of_size(g, 3, far_sem).wait_recv()
            to_partner(g, (3, -3, 4))

        by_carrier(g, act)

    def weights_done(g):
        by_carrier(g, lambda: of_size(g, 7, d2d_sem).wait_recv(), other=True)

    def project(i, q, fbuf):
        start = i * BLK + q * DOT
        if not isinstance(start, int):
            start = pl.multiple_of(start, 32)
        first = xv[pl.ds(start, DOT), :]
        second = xv[pl.ds(start + PAIRS, DOT), :]
        y = jnp.dot(jnp.concatenate([first, second], axis=1), waug[...], preferred_element_type=F32)
        lower = lax.broadcasted_iota(jnp.int32, (16, 128), 1) < DH

        def square_sums(row):
            total = None
            for c in range(0, D, 128):
                tile = xv[pl.ds(row, 16), c : c + 128].astype(F32)
                total = tile * tile if total is None else total + tile * tile
            return jnp.broadcast_to(jnp.sum(total, axis=1, keepdims=True), (16, 128))

        for r in range(0, DOT, SUB):
            rows = slice(r, r + SUB)
            squares = []
            for k in range(r, r + SUB, 16):
                row = start + k if isinstance(start, int) else pl.multiple_of(start + k, 16)
                other = row + PAIRS if isinstance(start, int) else pl.multiple_of(row + PAIRS, 16)
                squares.append(jnp.where(lower, square_sums(row), square_sums(other)))
            squares = jnp.concatenate(squares, axis=0)
            mean = y[rows, 128:256]
            var = jnp.maximum(squares * (1.0 / D) - mean * mean, 0.0)
            feats = (y[rows, 0:128] - cs[...] * mean) * lax.rsqrt(var + 1e-05)
            fbuf[q * DOT + r : q * DOT + r + SUB, :] = feats.astype(BF16)
            yield

    def slices(fbuf):
        logits = contract_lanes(pT[...], fbuf[...])
        yield
        exps = []
        for top in (0, G + 16):
            scaled = logits[top : top + G] * inverse_temperature(
                logits[top + G : top + G + 1] + logits[top + G + 1 : top + G + 2]
            )
            exps.append(jnp.exp(scaled - jnp.max(scaled, axis=0, keepdims=True)))
        yield
        w = [(e * (1.0 / jnp.sum(e, axis=0, keepdims=True))).astype(BF16) for e in exps]
        yield
        with_ones = jnp.concatenate([fbuf[...], jnp.ones((PAIRS, 128), BF16)], axis=1)
        acc[...] += jnp.dot(jnp.concatenate(w, axis=0), with_ones, preferred_element_type=F32)
        yield

    def project_and_slices(i, fbuf, other):
        steps = slices(other)
        for q in range(PAIRS // DOT):
            for _ in project(i, q, fbuf):
                next(steps)

    x_copy(0).wait()
    for q in range(PAIRS // DOT):
        for _ in project(0, q, f0):
            pass

    start_at = (z < 1).astype(jnp.int32) + (z < 4).astype(jnp.int32)

    def two_blocks(j, _):
        @pl.when(j == start_at)
        def _():
            pl.semaphore_wait(barrier, 1 + 15 + 7)
            weights_1()

        x_copy(2 * j + 1).wait()
        x_copy(2 * j + 2).wait()
        project_and_slices(2 * j + 1, f1, f0)
        project_and_slices(2 * j + 2, f0, f1)
        return 0

    lax.fori_loop(0, NBLK // 2 - 1, two_blocks, 0)
    weights_2(0)
    weights_2(1)
    x_copy(NBLK - 1).wait()
    project_and_slices(NBLK - 1, f1, f0)
    weights_2(2)
    weights_2(3)
    for _ in slices(f1):
        pass

    half_g = G // 2
    lane = lax.broadcasted_iota(jnp.int32, (G, 128), 1)
    diagonal = lane == lax.broadcasted_iota(jnp.int32, (G, 128), 0)
    even, odd = acc[0:G, 0:128], acc[G:, 0:128]
    straight, crossed = even + pltpu.roll(odd, DH, axis=1), pltpu.roll(even, DH, axis=1) + odd
    mass = acc[0:G, 128:256] + acc[G:, 128:256]
    pair[0, 0:half_g, :] = jnp.where(lane[0:half_g] < DH, straight[0:half_g], crossed[half_g:])
    pair[0, half_g : half_g + 1, :] = jnp.sum(jnp.where(diagonal, mass, 0.0), axis=0, keepdims=True)
    pair_copy = to(pair.at[0], pair_sem, (partner, z), pair.at[1])
    plane_all = to(plane.at[pl.ds(1, 15)], plane_sem, (partner, z))

    @pl.when(core == 0)
    def _():
        pair_copy.start()

    @pl.when(core == 1)
    def _():
        pair_copy.wait_recv()
        plane[0] = pair[0] + pair[1]
        for r in range(1, 16):
            to(plane.at[0], plane_sem, (pts_at(*PLANE[r]), z), plane.at[r]).start()

    weights_3(0)
    own = pl.multiple_of(z * OWN, 128)

    def own_norm(t, _):
        rows = xv[pl.ds(pl.multiple_of(own + t * NORM_ROWS, 32), NORM_ROWS), :].astype(F32)
        centred = rows - jnp.mean(rows, axis=1, keepdims=True)
        var = jnp.mean(centred * centred, axis=1, keepdims=True)
        nown[pl.ds(pl.multiple_of(t * NORM_ROWS, 32), NORM_ROWS), :] = (centred * lax.rsqrt(var + 1e-05)).astype(BF16)
        return 0

    lax.fori_loop(0, OWN // NORM_ROWS, own_norm, 0)
    for g in range(1, 4):
        weights_3(g)

    qkv_copy.wait()

    @pl.when(core == 1)
    def _():
        plane_all.wait_recv()
        sums = jnp.sum(plane[...], axis=0)
        packed = sums[0:half_g]
        numerator = jnp.concatenate([packed, pltpu.roll(packed, DH, axis=1)], axis=0)[:, 0:DH]
        mass = jnp.sum(jnp.where(diagonal, sums[half_g : half_g + 1], 0.0), axis=1, keepdims=True)
        tokens = numerator / (mass + 1e-05)
        maps = jnp.concatenate([qkv_ref[0], qkv_ref[1], qkv_ref[2], qkv_ref[2]], axis=1)
        mapped = jnp.dot(tokens, maps, preferred_element_type=F32, precision=HIGH)
        scores = contract_lanes(mapped[:, 0:DH], mapped[:, DH : 2 * DH], precision=HIGH) * 0.125
        values = jnp.where((lane < DH) == (lax.rem(z, 2) == 0), mapped[:, 2 * DH : 4 * DH], 0.0)
        e = jnp.exp(scores - jnp.max(scores, axis=1, keepdims=True))
        attend = e / jnp.sum(e, axis=1, keepdims=True)
        zbuf[z] = jnp.dot(attend, values, preferred_element_type=F32, precision=HIGH).astype(BF16)

        for dz in range(1, H):
            to(zbuf.at[z], z_sem, (pts, z_at(dz))).start()

    def z_of(n):
        return to(zbuf.at[pl.ds(0, n)], z_sem, (partner, z))

    weights_far(0)
    weights_done(0)
    yall[...] = contract_lanes(wall[0].reshape(D, D), nown[...]).astype(BF16)
    weights_far(1)
    for h in range(H):
        if h == 2:
            weights_far(2)
        if h == 5:
            weights_far(3)
        logits = jnp.dot(pT[0 : G + 16, 0:DH], yall[h * DH : (h + 1) * DH, :], preferred_element_type=F32)
        wT[h * G : (h + 1) * G, :] = softmax_weights(logits)
    wn[...] = wT[...].T
    @pl.when(core == 1)
    def _():
        z_of(H - 1).wait_recv()
        to(zbuf, z_sem, (partner, z)).start()

    @pl.when(core == 0)
    def _():
        z_of(H).wait_recv()

    weights_done(1)

    gap = jnp.zeros((2 * G, 128), BF16)
    for h in range(0, H, 4):
        first, second = (zbuf[k : k + 2].reshape(2 * G, 128) for k in (h, h + 2))
        tokens_of_four = jnp.concatenate(
            [jnp.concatenate([first, gap], axis=1), jnp.concatenate([gap, second], axis=1)], axis=0
        )
        mbuf[h * G : (h + 4) * G, :] = jnp.dot(
            tokens_of_four, wall[1, h : h + 4].reshape(4 * DH, D), preferred_element_type=F32
        ).astype(BF16)

    def mix(t, mid, normed):
        x_rows = xv[pl.ds(pl.multiple_of(own + t * TBLK, 32), TBLK), :].astype(F32)
        midway = x_rows + jnp.dot(wn[t * TBLK : (t + 1) * TBLK, :], mbuf[...], preferred_element_type=F32)
        centred = midway - jnp.mean(midway, axis=1, keepdims=True)
        var = jnp.mean(centred * centred, axis=1, keepdims=True)
        mid[...] = midway
        normed[...] = (centred * lax.rsqrt(var + 1e-05)).astype(BF16)

    def feed(t, mid, normed):
        hidden = jnp.dot(normed[...], wall[2].reshape(D, D), preferred_element_type=F32)
        hidden = jax.nn.gelu(hidden).astype(BF16)
        out = mid[...] + jnp.dot(hidden, wall[3].reshape(D, D), preferred_element_type=F32)
        out_ref[t * TBLK : (t + 1) * TBLK, :] = out.astype(BF16)

    stage = ((m0, n0), (m1, n1))
    mix(0, *stage[0])
    weights_done(2)
    weights_done(3)
    for t in range(OWN // TBLK):
        if t + 1 < OWN // TBLK:
            mix(t + 1, *stage[(t + 1) % 2])
        feed(t, *stage[t % 2])

    for g in range(4):

        def sent(g=g):
            of_size(g, 2, own_sem).wait_send()
            of_size(g, 2, hop_sem).wait_send()
            of_size(g, 3, far_sem).wait_send()
            of_size(g, 7, d2d_sem).wait_send()

        by_carrier(g, sent)

    @pl.when(core == 0)
    def _():
        pair_copy.wait_send()

    @pl.when(core == 1)
    def _():
        plane_all.wait_send()
        z_of(H).wait_send()
        z_of(H - 1).wait_send()


OUT = pltpu.VMEM((OWN, D), BF16)


def local(x, entry, partition, sharpness, qkv, exit_matrix, widening, narrowing):
    hbm = pl.BlockSpec(memory_space=pl.ANY)
    vmem = pl.BlockSpec(memory_space=pltpu.VMEM)
    dma = pltpu.SemaphoreType.DMA
    return pl.pallas_call(
        kernel,
        out_shape=OUT,
        in_specs=[hbm] * 8,
        out_specs=vmem,
        scratch_shapes=[
            pltpu.VMEM((ROWS, D), BF16),
            pltpu.VMEM((DH, D), BF16),
            pltpu.VMEM((G, DH), BF16),
            pltpu.VMEM((1, DH), F32),
            pltpu.VMEM((3, DH, DH), F32),
            pltpu.VMEM((2 * D, 256), BF16),
            pltpu.VMEM((2 * (G + 16), 128), BF16),
            pltpu.VMEM((1, 128), F32),
            pltpu.VMEM((PAIRS, 128), BF16),
            pltpu.VMEM((PAIRS, 128), BF16),
            pltpu.VMEM((2 * G, 256), F32),
            pltpu.VMEM((4, H, 2, HALF, D), BF16),
            pltpu.VMEM((OWN, D), BF16),
            pltpu.VMEM((H * G, OWN), BF16),
            pltpu.VMEM((OWN, H * G), BF16),
            pltpu.VMEM((H * G, D), BF16),
            pltpu.VMEM((D, OWN), BF16),
            pltpu.VMEM((TBLK, D), F32),
            pltpu.VMEM((TBLK, D), F32),
            pltpu.VMEM((TBLK, D), BF16),
            pltpu.VMEM((TBLK, D), BF16),
            pltpu.VMEM((2, G // 2 + 1, 128), F32),
            pltpu.VMEM((16, G // 2 + 1, 128), F32),
            pltpu.VMEM((H, G, 128), BF16),
            dma((NBLK,)),
            dma((12,)),
            dma((4, 2)),
            dma((4, 2)),
            dma((4, 2)),
            dma((4, 2)),
            dma((2,)),
            dma((2,)),
            dma((2,)),
        ],
        compiler_params=pltpu.CompilerParams(
            collective_id=0, has_side_effects=True, vmem_limit_bytes=60 * 2**20
        ),
    )(x, entry.T, partition.T, sharpness.reshape(1, DH), qkv, exit_matrix, widening, narrowing)


def solution(mesh):
    placed = (
        P("pts", None), P(None, "wid"), P(), P(), P(),
        P("wid", None), P("wid", None), P("wid", None),
    )
    return jax.shard_map(
        local, mesh=mesh, in_specs=placed, out_specs=P(("pts", "wid"), None), check_vma=False
    )
```

```python
import functools

import jax
import jax.numpy as jnp
from jax import lax
from jax.experimental import pallas as pl
from jax.experimental.pallas import tpu as pltpu
from jax.sharding import PartitionSpec as P

MESH = pl.DeviceIdType.MESH
F32, BF16 = jnp.float32, jnp.bfloat16
HIGH = lax.Precision.HIGHEST

D, H, DH, G = 512, 8, 64, 32
ROWS = 11264
OWN = 1408
BLK = 1408
PAIRS = BLK // 2
DOT = 352
SUB = 176
NBLK = ROWS // BLK
NORM_ROWS = 352
TBLK = 704
HALF = DH // 2

PLANE = [(dx, dy) for dx in range(4) for dy in range(4)]


def contract_lanes(a, b, precision=None):
    return lax.dot_general(
        a, b, (((1,), (1,)), ((), ())), preferred_element_type=F32, precision=precision
    )


def inverse_temperature(logit):
    return 1.0 / (0.5 + jnp.maximum(logit, 0.0) + jnp.log(1.0 + jnp.exp(-jnp.abs(logit))))


def softmax_weights(logits):
    scaled = logits[0:G] * inverse_temperature(logits[G : G + 1] + logits[G + 1 : G + 2])
    e = jnp.exp(scaled - jnp.max(scaled, axis=0, keepdims=True))
    return (e * (1.0 / jnp.sum(e, axis=0, keepdims=True))).astype(BF16)


def kernel(
    x_hbm, entry_hbm, part_hbm, sharp_hbm, qkv_hbm, exit_hbm, wide_hbm, narrow_hbm,
    out_ref,
    xv, eh, part_ref, sharp_ref, qkv_ref, waug, pT, cs, f0, f1, acc, wall, nown, wT, wn, mbuf, yall, m0, m1, n0, n1,
    pair, plane, zbuf,
    x_sem, in_sem, own_sem, hop_sem, far_sem, d2d_sem, pair_sem, plane_sem, z_sem,
):
    pts, z = lax.axis_index("pts"), lax.axis_index("wid")
    core = lax.rem(pts, 2)
    gx, gy = pts // 8, lax.rem(pts // 2, 4)
    partner = pts + 1 - 2 * core

    def pts_at(dx, dy):
        return (lax.rem(gx + dx, 4) * 4 + lax.rem(gy + dy, 4)) * 2 + core

    def z_at(dz):
        return lax.rem(z + dz + H, H)

    def x_copy(i):
        return pltpu.make_async_copy(
            x_hbm.at[pl.ds(i * BLK, BLK)], xv.at[pl.ds(i * BLK, BLK)], x_sem.at[i]
        )

    entry_copy = pltpu.make_async_copy(entry_hbm, eh, in_sem.at[0])
    small_copies = [
        pltpu.make_async_copy(part_hbm, part_ref, in_sem.at[9]),
        pltpu.make_async_copy(sharp_hbm, sharp_ref, in_sem.at[10]),
    ]
    qkv_copy = pltpu.make_async_copy(qkv_hbm, qkv_ref, in_sem.at[11])
    entry_copy.start()
    for copy in small_copies:
        copy.start()
    x_copy(0).start()
    own_copies = []
    for k, ref in enumerate((entry_hbm, exit_hbm, wide_hbm, narrow_hbm)):
        for c in range(2):
            own_copies.append(
                pltpu.make_async_copy(
                    ref.at[pl.ds(c * HALF, HALF)], wall.at[k, z, c], in_sem.at[1 + 2 * k + c]
                )
            )

    for copy in own_copies:
        copy.start()
    qkv_copy.start()

    barrier = pltpu.get_barrier_semaphore()
    pl.semaphore_signal(barrier, inc=1, device_id=(partner, z), device_id_type=MESH)
    for dx, dy in PLANE[1:]:
        pl.semaphore_signal(barrier, inc=1, device_id=(pts_at(dx, dy), z), device_id_type=MESH)
    for dz in range(1, H):
        pl.semaphore_signal(barrier, inc=1, device_id=(pts, z_at(dz)), device_id_type=MESH)

    for copy in small_copies:
        copy.wait()
    sharp = jnp.broadcast_to(sharp_ref[...], (16, DH))
    sharp_hi = sharp.astype(BF16).astype(F32)
    row16 = lax.broadcasted_iota(jnp.int32, (16, DH), 0)
    tail = jnp.where(row16 == 0, sharp_hi, jnp.where(row16 == 1, sharp - sharp_hi, 0.0))
    table = jnp.concatenate([part_ref[...].astype(F32), tail], axis=0)
    blank = jnp.zeros((G + 16, DH), F32)
    pT[0 : G + 16, :] = jnp.concatenate([table, blank], axis=1).astype(BF16)
    pT[G + 16 :, :] = jnp.concatenate([blank, table], axis=1).astype(BF16)
    acc[...] = jnp.zeros_like(acc)

    for i in range(1, NBLK):
        x_copy(i).start()
    entry_copy.wait()
    head = eh[...].astype(F32)
    low = lax.broadcasted_iota(jnp.int32, (D, 128), 1) < DH
    both = jnp.concatenate([head, head], axis=0).T
    cs[...] = jnp.sum(both, axis=0, keepdims=True)
    for half, lanes in ((0, low), (1, jnp.logical_not(low))):
        waug[half * D : (half + 1) * D, 0:128] = jnp.where(lanes, both, 0.0).astype(BF16)
        waug[half * D : (half + 1) * D, 128:256] = jnp.where(lanes, 1.0 / D, 0.0).astype(BF16)

    carrier = {0: 1, 1: 0, 2: 1, 3: 0}

    def to(ref, sems, device, target=None):
        return pltpu.make_async_remote_copy(
            src_ref=ref, dst_ref=ref if target is None else target, send_sem=sems.at[0], recv_sem=sems.at[1],
            device_id=device, device_id_type=MESH,
        )

    def by_carrier(g, act, other=False):
        if g in carrier:
            pl.when(core == (1 - carrier[g] if other else carrier[g]))(act)
        else:
            act()

    def piece(g, offset, side=None):
        shard = z_at(offset)
        if g in carrier:
            return wall.at[g, shard] if side is None else wall.at[g, shard, side]
        rows = pl.ds(0, HALF) if side is None else pl.ds(side * (HALF // 2), HALF // 2)
        return wall.at[g, shard, core, rows]

    def of_size(g, n, sems):
        some = wall.at[g, pl.ds(0, n)] if g in carrier else wall.at[g, pl.ds(0, n), 0]
        return to(some, sems.at[g], (partner, z))

    def to_partner(g, offsets):
        for offset in offsets:
            to(piece(g, offset), d2d_sem.at[g], (partner, z)).start()

    def weights_1():
        for copy in own_copies:
            copy.wait()
        for g in range(4):

            def act(g=g):
                for d in (1, -1):
                    to(piece(g, 0), own_sem.at[g], (pts, z_at(d))).start()

            by_carrier(g, act)

    def weights_2(g):
        def act():
            of_size(g, 2, own_sem).wait_recv()
            for d in (1, -1):
                to(piece(g, -d), hop_sem.at[g], (pts, z_at(d))).start()

        by_carrier(g, act)

    def weights_3(g):
        def act():
            of_size(g, 2, hop_sem).wait_recv()
            for d, side in ((1, 0), (-1, 1)):
                to(piece(g, -2 * d), far_sem.at[g], (pts, z_at(d))).start()
                to(piece(g, -2 * d, side), far_sem.at[g], (pts, z_at(2 * d))).start()
            to_partner(g, (1, -1, 2, -2))

        by_carrier(g, act)

    def weights_far(g):
        def act():
            of_size(g, 3, far_sem).wait_recv()
            to_partner(g, (3, -3, 4))

        by_carrier(g, act)

    def weights_done(g):
        by_carrier(g, lambda: of_size(g, 7, d2d_sem).wait_recv(), other=True)

    def project(i, q, fbuf):
        start = i * BLK + q * DOT
        if not isinstance(start, int):
            start = pl.multiple_of(start, 32)
        first = xv[pl.ds(start, DOT), :]
        second = xv[pl.ds(start + PAIRS, DOT), :]
        y = jnp.dot(jnp.concatenate([first, second], axis=1), waug[...], preferred_element_type=F32)
        lower = lax.broadcasted_iota(jnp.int32, (16, 128), 1) < DH

        def square_sums(row):
            total = None
            for c in range(0, D, 128):
                tile = xv[pl.ds(row, 16), c : c + 128].astype(F32)
                total = tile * tile if total is None else total + tile * tile
            return jnp.broadcast_to(jnp.sum(total, axis=1, keepdims=True), (16, 128))

        for r in range(0, DOT, SUB):
            rows = slice(r, r + SUB)
            squares = []
            for k in range(r, r + SUB, 16):
                row = start + k if isinstance(start, int) else pl.multiple_of(start + k, 16)
                other = row + PAIRS if isinstance(start, int) else pl.multiple_of(row + PAIRS, 16)
                squares.append(jnp.where(lower, square_sums(row), square_sums(other)))
            squares = jnp.concatenate(squares, axis=0)
            mean = y[rows, 128:256]
            var = jnp.maximum(squares * (1.0 / D) - mean * mean, 0.0)
            feats = (y[rows, 0:128] - cs[...] * mean) * lax.rsqrt(var + 1e-05)
            fbuf[q * DOT + r : q * DOT + r + SUB, :] = feats.astype(BF16)
            yield

    def slices(fbuf):
        logits = contract_lanes(pT[...], fbuf[...])
        yield
        exps = []
        for top in (0, G + 16):
            scaled = logits[top : top + G] * inverse_temperature(
                logits[top + G : top + G + 1] + logits[top + G + 1 : top + G + 2]
            )
            exps.append(jnp.exp(scaled - jnp.max(scaled, axis=0, keepdims=True)))
        yield
        w = [(e * (1.0 / jnp.sum(e, axis=0, keepdims=True))).astype(BF16) for e in exps]
        yield
        with_ones = jnp.concatenate([fbuf[...], jnp.ones((PAIRS, 128), BF16)], axis=1)
        acc[...] += jnp.dot(jnp.concatenate(w, axis=0), with_ones, preferred_element_type=F32)
        yield

    def project_and_slices(i, fbuf, other):
        steps = slices(other)
        for q in range(PAIRS // DOT):
            for _ in project(i, q, fbuf):
                next(steps)

    x_copy(0).wait()
    for q in range(PAIRS // DOT):
        for _ in project(0, q, f0):
            pass

    start_at = (z < 1).astype(jnp.int32) + (z < 3).astype(jnp.int32)

    def two_blocks(j, _):
        @pl.when(j == start_at)
        def _():
            pl.semaphore_wait(barrier, 1 + 15 + 7)
            weights_1()

        x_copy(2 * j + 1).wait()
        x_copy(2 * j + 2).wait()
        project_and_slices(2 * j + 1, f1, f0)
        project_and_slices(2 * j + 2, f0, f1)
        return 0

    lax.fori_loop(0, NBLK // 2 - 1, two_blocks, 0)
    weights_2(0)
    weights_2(1)
    x_copy(NBLK - 1).wait()
    project_and_slices(NBLK - 1, f1, f0)
    weights_2(2)
    weights_2(3)
    for _ in slices(f1):
        pass

    half_g = G // 2
    lane = lax.broadcasted_iota(jnp.int32, (G, 128), 1)
    diagonal = lane == lax.broadcasted_iota(jnp.int32, (G, 128), 0)
    even, odd = acc[0:G, 0:128], acc[G:, 0:128]
    straight, crossed = even + pltpu.roll(odd, DH, axis=1), pltpu.roll(even, DH, axis=1) + odd
    mass = acc[0:G, 128:256] + acc[G:, 128:256]
    pair[0, 0:half_g, :] = jnp.where(lane[0:half_g] < DH, straight[0:half_g], crossed[half_g:])
    pair[0, half_g : half_g + 1, :] = jnp.sum(jnp.where(diagonal, mass, 0.0), axis=0, keepdims=True)
    pair_copy = to(pair.at[0], pair_sem, (partner, z), pair.at[1])
    plane_all = to(plane.at[pl.ds(1, 15)], plane_sem, (partner, z))

    @pl.when(core == 0)
    def _():
        pair_copy.start()

    @pl.when(core == 1)
    def _():
        pair_copy.wait_recv()
        plane[0] = pair[0] + pair[1]
        for r in range(1, 16):
            to(plane.at[0], plane_sem, (pts_at(*PLANE[r]), z), plane.at[r]).start()

    weights_3(0)
    own = pl.multiple_of(z * OWN, 128)

    def own_norm(t, _):
        rows = xv[pl.ds(pl.multiple_of(own + t * NORM_ROWS, 32), NORM_ROWS), :].astype(F32)
        centred = rows - jnp.mean(rows, axis=1, keepdims=True)
        var = jnp.mean(centred * centred, axis=1, keepdims=True)
        nown[pl.ds(pl.multiple_of(t * NORM_ROWS, 32), NORM_ROWS), :] = (centred * lax.rsqrt(var + 1e-05)).astype(BF16)
        return 0

    lax.fori_loop(0, OWN // NORM_ROWS, own_norm, 0)
    for g in range(1, 4):
        weights_3(g)

    qkv_copy.wait()

    @pl.when(core == 1)
    def _():
        plane_all.wait_recv()
        sums = jnp.sum(plane[...], axis=0)
        packed = sums[0:half_g]
        numerator = jnp.concatenate([packed, pltpu.roll(packed, DH, axis=1)], axis=0)[:, 0:DH]
        mass = jnp.sum(jnp.where(diagonal, sums[half_g : half_g + 1], 0.0), axis=1, keepdims=True)
        tokens = numerator / (mass + 1e-05)
        maps = jnp.concatenate([qkv_ref[0], qkv_ref[1], qkv_ref[2], qkv_ref[2]], axis=1)
        mapped = jnp.dot(tokens, maps, preferred_element_type=F32, precision=HIGH)
        scores = contract_lanes(mapped[:, 0:DH], mapped[:, DH : 2 * DH], precision=HIGH) * 0.125
        values = jnp.where((lane < DH) == (lax.rem(z, 2) == 0), mapped[:, 2 * DH : 4 * DH], 0.0)
        e = jnp.exp(scores - jnp.max(scores, axis=1, keepdims=True))
        attend = e / jnp.sum(e, axis=1, keepdims=True)
        zbuf[z] = jnp.dot(attend, values, preferred_element_type=F32, precision=HIGH).astype(BF16)

        for dz in range(1, H):
            to(zbuf.at[z], z_sem, (pts, z_at(dz))).start()

    def z_of(n):
        return to(zbuf.at[pl.ds(0, n)], z_sem, (partner, z))

    weights_far(0)
    weights_done(0)
    yall[...] = contract_lanes(wall[0].reshape(D, D), nown[...]).astype(BF16)
    weights_far(1)
    for h in range(H):
        if h == 2:
            weights_far(2)
        if h == 5:
            weights_far(3)
        logits = jnp.dot(pT[0 : G + 16, 0:DH], yall[h * DH : (h + 1) * DH, :], preferred_element_type=F32)
        wT[h * G : (h + 1) * G, :] = softmax_weights(logits)
    wn[...] = wT[...].T
    @pl.when(core == 1)
    def _():
        z_of(H - 1).wait_recv()
        to(zbuf, z_sem, (partner, z)).start()

    @pl.when(core == 0)
    def _():
        z_of(H).wait_recv()

    weights_done(1)

    gap = jnp.zeros((2 * G, 128), BF16)
    for h in range(0, H, 4):
        first, second = (zbuf[k : k + 2].reshape(2 * G, 128) for k in (h, h + 2))
        tokens_of_four = jnp.concatenate(
            [jnp.concatenate([first, gap], axis=1), jnp.concatenate([gap, second], axis=1)], axis=0
        )
        mbuf[h * G : (h + 4) * G, :] = jnp.dot(
            tokens_of_four, wall[1, h : h + 4].reshape(4 * DH, D), preferred_element_type=F32
        ).astype(BF16)

    def mix(t, mid, normed):
        x_rows = xv[pl.ds(pl.multiple_of(own + t * TBLK, 32), TBLK), :].astype(F32)
        midway = x_rows + jnp.dot(wn[t * TBLK : (t + 1) * TBLK, :], mbuf[...], preferred_element_type=F32)
        centred = midway - jnp.mean(midway, axis=1, keepdims=True)
        var = jnp.mean(centred * centred, axis=1, keepdims=True)
        mid[...] = midway
        normed[...] = (centred * lax.rsqrt(var + 1e-05)).astype(BF16)

    def feed(t, mid, normed):
        hidden = jnp.dot(normed[...], wall[2].reshape(D, D), preferred_element_type=F32)
        hidden = jax.nn.gelu(hidden).astype(BF16)
        out = mid[...] + jnp.dot(hidden, wall[3].reshape(D, D), preferred_element_type=F32)
        out_ref[t * TBLK : (t + 1) * TBLK, :] = out.astype(BF16)

    stage = ((m0, n0), (m1, n1))
    mix(0, *stage[0])
    weights_done(2)
    weights_done(3)
    for t in range(OWN // TBLK):
        if t + 1 < OWN // TBLK:
            mix(t + 1, *stage[(t + 1) % 2])
        feed(t, *stage[t % 2])

    for g in range(4):

        def sent(g=g):
            of_size(g, 2, own_sem).wait_send()
            of_size(g, 2, hop_sem).wait_send()
            of_size(g, 3, far_sem).wait_send()
            of_size(g, 7, d2d_sem).wait_send()

        by_carrier(g, sent)

    @pl.when(core == 0)
    def _():
        pair_copy.wait_send()

    @pl.when(core == 1)
    def _():
        plane_all.wait_send()
        z_of(H).wait_send()
        z_of(H - 1).wait_send()


OUT = pltpu.VMEM((OWN, D), BF16)


def local(x, entry, partition, sharpness, qkv, exit_matrix, widening, narrowing):
    hbm = pl.BlockSpec(memory_space=pl.ANY)
    vmem = pl.BlockSpec(memory_space=pltpu.VMEM)
    dma = pltpu.SemaphoreType.DMA
    return pl.pallas_call(
        kernel,
        out_shape=OUT,
        in_specs=[hbm] * 8,
        out_specs=vmem,
        scratch_shapes=[
            pltpu.VMEM((ROWS, D), BF16),
            pltpu.VMEM((DH, D), BF16),
            pltpu.VMEM((G, DH), BF16),
            pltpu.VMEM((1, DH), F32),
            pltpu.VMEM((3, DH, DH), F32),
            pltpu.VMEM((2 * D, 256), BF16),
            pltpu.VMEM((2 * (G + 16), 128), BF16),
            pltpu.VMEM((1, 128), F32),
            pltpu.VMEM((PAIRS, 128), BF16),
            pltpu.VMEM((PAIRS, 128), BF16),
            pltpu.VMEM((2 * G, 256), F32),
            pltpu.VMEM((4, H, 2, HALF, D), BF16),
            pltpu.VMEM((OWN, D), BF16),
            pltpu.VMEM((H * G, OWN), BF16),
            pltpu.VMEM((OWN, H * G), BF16),
            pltpu.VMEM((H * G, D), BF16),
            pltpu.VMEM((D, OWN), BF16),
            pltpu.VMEM((TBLK, D), F32),
            pltpu.VMEM((TBLK, D), F32),
            pltpu.VMEM((TBLK, D), BF16),
            pltpu.VMEM((TBLK, D), BF16),
            pltpu.VMEM((2, G // 2 + 1, 128), F32),
            pltpu.VMEM((16, G // 2 + 1, 128), F32),
            pltpu.VMEM((H, G, 128), BF16),
            dma((NBLK,)),
            dma((12,)),
            dma((4, 2)),
            dma((4, 2)),
            dma((4, 2)),
            dma((4, 2)),
            dma((2,)),
            dma((2,)),
            dma((2,)),
        ],
        compiler_params=pltpu.CompilerParams(
            collective_id=0, has_side_effects=True, vmem_limit_bytes=60 * 2**20
        ),
    )(x, entry.T, partition.T, sharpness.reshape(1, DH), qkv, exit_matrix, widening, narrowing)


def solution(mesh):
    placed = (
        P("pts", None), P(None, "wid"), P(), P(), P(),
        P("wid", None), P("wid", None), P("wid", None),
    )
    return jax.shard_map(
        local, mesh=mesh, in_specs=placed, out_specs=P(("pts", "wid"), None), check_vma=False
    )
```
